32 devices in a mesh: groups: 2 (over x), gx: 16 (over z, y, core).
Axes of the slice: x: 2, y: 2, z: 4, core: 2. Of those that a mesh axis runs over, the one named last changes fastest.
Arguments:
- points: bfloat16 [32, 6, 1, 128, 512], P(('groups', 'gx')), parts along dimension 0, may hold values from -6 to 6
- order: int32 [32, 6, 1, 128], P(('groups', 'gx')), parts along dimension 0, may hold values from 0 to 127, each once within a row
- masks: int32 [32, 6, 1, 26], P(('groups', 'gx')), parts along dimension 0, may hold values 0 or 1
- counts: int32 [32, 6, 1], P('groups'), parts along dimension 0, may hold values from 1 to 128
- gain: float32 [512], replicated, may hold values from 0.5 to 1.5
- shift_bias: float32 [512], replicated, may hold values from -3 to 3
- w_qkv: bfloat16 [512, 1536], replicated, may hold values from -1.5 to 1.5
- w_out: bfloat16 [512, 512], replicated, may hold values from -0.25 to 0.25
Outputs:
- result: bfloat16 [32, 6, 1, 128, 512], P(('groups', 'gx')), parts along dimension 0
The draws below stay inside these ranges and needn't reach their ends.
There are 2 independent parts, one for each index of `groups`. The reference program is written for one: setup_inputs(seed, part) draws one part's arguments, and reference() takes and returns one part's arrays. A program takes and returns all parts, laid end to end along the dimension named above; an argument that names none is the same for every part. Nothing has to cross between parts.
All inputs are finite; a program needn't handle non-finite values. No bound on the sum of `masks` on one device may be relied on, other than what follows from the above.
Results may differ from the reference program's by a relative error of at most 0.012.
Values may be sent and summed in bfloat16 or wider, within the bound.
A program may use at most 128 MiB of HBM per device.

```python
import jax
import jax.numpy as jnp
from jax import lax

D = 512
HEADS = 8
P_SIZE = 128
BY = 6
BZ = 1
NBX = 16


def bias_normal(key):
    values = jax.random.normal(jax.random.fold_in(key, 1701), (D,), jnp.float32)
    return jnp.clip(values, -6.0, 6.0)


def draw_shift_bias(key, part):
    return 0.5 * bias_normal(key)


def draw_w_qkv(key, part):
    spread = D ** (-0.5)
    noise = jax.random.normal(jax.random.fold_in(key, 1702), (D, 3 * D), jnp.float32) * spread
    noise = jnp.clip(noise, -6.0 * spread, 6.0 * spread)
    return noise.astype(jnp.bfloat16)


def plant(drawn, stream_key, least, top_value):
    shape = drawn.shape
    index_at = [jax.random.randint(jax.random.fold_in(stream_key, axis), (), 0, shape[axis]) for axis in range(len(shape))]
    drawn = drawn.at[tuple(index_at)].set(least)
    longest = shape.index(max(shape))
    index_at[longest] = (index_at[longest] + 1) % shape[longest]
    return drawn.at[tuple(index_at)].set(top_value)


def steps_of(own_key, dims, pieces, low, top_value):
    level, own = 1.0, jax.random.fold_in(own_key, 6)
    for position, parts in pieces:
        heights = jnp.exp(jax.random.uniform(jax.random.fold_in(own, position), (parts,), jnp.float32, low / len(pieces), top_value / len(pieces)))
        level = level * jnp.repeat(heights, dims[position] // parts).reshape([-1 if axis == position else 1 for axis in range(len(dims))])
    return level


def centred(key, extent, deviation, bound, split=(), kind=jnp.bfloat16):
    level = steps_of(key, extent, split, -0.22, 0.18) if split else 1.0
    array = jax.random.normal(key, extent, jnp.float32) * deviation * level
    return jnp.minimum(jnp.maximum(array, -bound), bound).astype(kind)


def setup_inputs(seed: int = 0, part: int = 0) -> dict:
    keys = jax.random.split(jax.random.key(seed), 9)
    part_splits = jax.random.split(jax.random.fold_in(keys[8], part), 9)
    points = centred(part_splits[0], (NBX, BY, BZ, P_SIZE, D), 1.0, 6.0, ((0, 16),))
    order = jax.vmap(lambda own: jax.random.permutation(own, P_SIZE))(jax.random.split(part_splits[1], NBX * BY * BZ)).reshape((NBX, BY, BZ, P_SIZE)).astype(jnp.int32)
    masks = plant((jax.random.randint(part_splits[2], (NBX, BY, BZ, 26), 0, 2) < 1).astype(jnp.int32), jax.random.fold_in(part_splits[2], 1), 0, 1)
    counts = plant(jax.random.randint(part_splits[3], (NBX, BY, BZ), 1, P_SIZE + 1), jax.random.fold_in(part_splits[3], 1), 1, P_SIZE).astype(jnp.int32)
    gain = jnp.clip(1.0 + 0.1 * jax.random.normal(keys[4], (D,), jnp.float32), 0.5, 1.5)
    shift_bias = draw_shift_bias(jax.random.fold_in(keys[8], 71), part)
    w_qkv = draw_w_qkv(jax.random.fold_in(keys[8], 71), part)
    w_out = centred(keys[7], (D, D), D ** -0.5, 0.25)
    return dict(points=points, order=order, masks=masks, counts=counts, gain=gain, shift_bias=shift_bias, w_qkv=w_qkv, w_out=w_out)


neighbour_offsets = [(a, b, c) for a in (-1, 0, 1) for b in (-1, 0, 1) for c in (-1, 0, 1)]

def column_of(a, b, c):
    index = 9 * (a + 1) + 3 * (b + 1) + (c + 1)
    return index if index < 13 else index - 1

def layer_norm(tiled, gain, shift_bias):
    values = tiled.astype(jnp.float32)
    mean = lax.optimization_barrier(jnp.mean(values, axis=-1, keepdims=True))
    var = lax.optimization_barrier(jnp.mean((values - mean) ** 2, axis=-1, keepdims=True))
    return ((values - mean) * lax.rsqrt(var + 1e-05) * gain + shift_bias).astype(jnp.bfloat16)

def attend_slab(queries, slabs, counts_pad, masks, heads):
    by, bz, p, width = queries.shape
    hd = width // heads
    scale = 1.0 / hd ** 0.5
    positions = jnp.arange(p, dtype=jnp.int32)
    blocks = []
    valids = []
    for a, b, c in neighbour_offsets:
        block = slabs[a + 1][1 + b:1 + b + by, 1 + c:1 + c + bz]
        near = counts_pad[a + 1, 1 + b:1 + b + by, 1 + c:1 + c + bz]
        valid = positions[None, None, :] < near[:, :, None]
        if (a, b, c) != (0, 0, 0):
            valid = valid & (masks[:, :, column_of(a, b, c)][:, :, None] == 1)
        blocks.append(block)
        valids.append(valid)
    keyvals = jnp.concatenate(blocks, axis=2).reshape(by * bz, -1, 2 * width)
    valid = jnp.concatenate(valids, axis=2).reshape(by * bz, -1)
    flat_queries = queries.reshape(by * bz, p, width)

    def one_block(operands):
        query, keyval, mask = operands
        qh = query.reshape(p, heads, hd).astype(jnp.float32)
        kh = keyval[:, :width].reshape(-1, heads, hd).astype(jnp.float32)
        vh = keyval[:, width:].reshape(-1, heads, hd).astype(jnp.float32)
        scores = jnp.einsum('qhd,khd->hqk', qh, kh) * scale
        scores = jnp.where(mask[None, None, :], scores, -1e+30)
        top = lax.optimization_barrier(jnp.max(scores, axis=-1, keepdims=True))
        probs = jnp.where(mask[None, None, :], jnp.exp(scores - top), 0.0)
        total = lax.optimization_barrier(jnp.sum(probs, axis=-1))
        rounded = probs.astype(jnp.bfloat16).astype(jnp.float32)
        accum = jnp.einsum('hqk,khd->qhd', rounded, vh)
        return (accum / jnp.transpose(total)[..., None]).reshape(p, width)
    attn = lax.map(one_block, (flat_queries, keyvals, valid))
    return attn.reshape(by, bz, p, width).astype(jnp.bfloat16)

def reference(points, order, masks, counts, gain, shift_bias, w_qkv, w_out):
    nbx, by, bz, p, width = points.shape
    tiled = jnp.take_along_axis(points, order[..., None], axis=3)
    normed = layer_norm(tiled, gain, shift_bias)
    qkv = jnp.dot(normed.reshape(-1, width), w_qkv, preferred_element_type=jnp.float32).astype(jnp.bfloat16)
    qkv = qkv.reshape(nbx, by, bz, p, 3 * width)
    queries = qkv[..., :width]
    keyvals = jnp.pad(qkv[..., width:], ((1, 1), (1, 1), (1, 1), (0, 0), (0, 0)))
    counts_pad = jnp.pad(counts, 1)

    def one_slab(index):
        index = index.astype(jnp.int32)
        slab = lax.dynamic_slice_in_dim(keyvals, index, 3, 0)
        near = lax.dynamic_slice_in_dim(counts_pad, index, 3, 0)
        query = lax.dynamic_index_in_dim(queries, index, 0, keepdims=False)
        mask = lax.dynamic_index_in_dim(masks, index, 0, keepdims=False)
        return attend_slab(query, (slab[0], slab[1], slab[2]), near, mask, HEADS)
    attn = lax.map(one_slab, jnp.arange(nbx, dtype=jnp.int32))
    mixed = jnp.dot(attn.reshape(-1, width), w_out, preferred_element_type=jnp.float32).reshape(nbx, by, bz, p, width)
    mixed = tiled.astype(jnp.float32) + mixed
    live = jnp.arange(p, dtype=jnp.int32)[None, None, None, :] < counts[..., None]
    return jnp.where(live[..., None], mixed, 0.0).astype(jnp.bfloat16)
```

```python
import functools

import jax
import jax.numpy as jnp
from jax import lax
from jax.experimental import pallas as pl
from jax.experimental.pallas import tpu as pltpu
from jax.sharding import PartitionSpec as P

HEADS = 8
TILE = 256
PIECE = 32
SPAN = 4
NEG = -1e30


def column_of(a, b, c):
    index = 9 * (a + 1) + 3 * (b + 1) + (c + 1)
    return index if index < 13 else index - 1


def reach(by, bz):
    spans = [(b, c) for b in (0, -1, 1) for c in (0, -1, 1)]
    return [o for o in spans if (by > 1 or o[0] == 0) and (bz > 1 or o[1] == 0)]


def norm_kernel(dims, pts_hbm, order_hbm, gain_hbm, shift_hbm, w_hbm, w_out_hbm, tiled_ref,
                normed_ref, w_ref, w_out_ref, pts_ref, order_ref, gain_ref, shift_ref, pts_sem,
                sems):
    by, bz, p, width, n = dims
    nb = by * bz
    copies = [
        pltpu.make_async_copy(order_hbm, order_ref, sems.at[0]),
        pltpu.make_async_copy(gain_hbm, gain_ref, sems.at[1]),
        pltpu.make_async_copy(shift_hbm, shift_ref, sems.at[2]),
    ]
    copies += [
        pltpu.make_async_copy(pts_hbm.at[g], pts_ref.at[g], pts_sem.at[g]) for g in range(nb)
    ]
    later = [
        pltpu.make_async_copy(w_hbm, w_ref, sems.at[3]),
        pltpu.make_async_copy(w_out_hbm, w_out_ref, sems.at[4]),
    ]
    for copy in copies + later:
        copy.start()
    for copy in copies:
        copy.wait()
    for g in range(nb):
        row = order_ref[0, g // bz, g % bz : g % bz + 1, :]
        pick = lax.broadcasted_iota(jnp.int32, (p, p), 0) == row
        pick = jnp.where(pick, 1.0, 0.0).astype(jnp.bfloat16)
        tiled = lax.dot_general(
            pick, pts_ref[g], (((0,), (0,)), ((), ())), preferred_element_type=jnp.float32
        )
        tiled_ref[g] = tiled.astype(jnp.bfloat16)
        mean = jnp.mean(tiled, axis=-1, keepdims=True)
        away = tiled - mean
        var = jnp.mean(away * away, axis=-1, keepdims=True)
        normed = away * lax.rsqrt(var + 1e-05) * gain_ref[...] + shift_ref[...]
        normed_ref[g * p : (g + 1) * p, :] = normed.astype(jnp.bfloat16)
    for copy in later:
        copy.wait()


def project(normed_ref, w_ref, lo, hi, put):
    for col in range(lo, hi, TILE):
        part = jnp.dot(
            normed_ref[...], w_ref[:, col : col + TILE], preferred_element_type=jnp.float32
        )
        put(col, part)


def put_keys(kv_ref, base, width):
    def put(col, part):
        rows = part.shape[0]
        kv_ref[base : base + rows, col - width : col - width + TILE] = part.astype(jnp.bfloat16)

    return put


def plan(slabs, masks_ref, counts_ref, table_ref, owner_ref, by, bz, p):
    nb = by * bz
    counts = [
        [jnp.where(present, counts_ref[k // bz, k % bz, at], 0) for k in range(nb)]
        for _, at, present in slabs
    ]
    item = jnp.int32(0)
    for g in range(nb):
        j, l = g // bz, g % bz
        base = item * SPAN
        used = base
        near = [(b, c) for b, c in reach(by, bz) if 0 <= j + b < by and 0 <= l + c < bz]
        for s, (kind, _, _) in enumerate(slabs):
            for b, c in near:
                k = (j + b) * bz + l + c
                count = counts[s][k]
                if kind is not None:
                    col = jnp.where(kind, column_of(1, b, c), column_of(-1, b, c))
                    count = count * masks_ref[0, j, l, col]
                elif (b, c) != (0, 0):
                    count = count * masks_ref[0, j, l, column_of(0, b, c)]
                for t in range(p // PIECE):
                    table_ref[0, used + t] = (s * nb + k) * p + t * PIECE
                    table_ref[1, used + t] = count - t * PIECE
                used = used + lax.shift_right_logical(count + (PIECE - 1), PIECE.bit_length() - 1)
        for t in range(SPAN):
            table_ref[0, used + t] = 0
            table_ref[1, used + t] = 0
        most = len(slabs) * len(near) * (p // PIECE) // SPAN
        for t in range(most):
            owner_ref[item + t] = g
        item = item + lax.shift_right_logical(used - base + (SPAN - 1), SPAN.bit_length() - 1)
    for t in range(2):
        owner_ref[item + t] = nb - 1
        for k in range(SPAN):
            table_ref[0, (item + t) * SPAN + k] = 0
            table_ref[1, (item + t) * SPAN + k] = 0
    return item


def work(items, table_ref, owner_ref, kv_ref, qd_ref, s_ref, m_ref, l_ref, acc_ref, width, p):
    hd = width // HEADS
    pairs = HEADS // 2

    def look(t):
        starts = [pl.multiple_of(table_ref[0, t * SPAN + k], PIECE) for k in range(SPAN)]
        return starts, [table_ref[1, t * SPAN + k] for k in range(SPAN)], owner_ref[t]

    def lanes_of(both, i):
        return jnp.concatenate([both[2 * i : 2 * i + 1], both[2 * i + 1 : 2 * i + 2]], axis=1)

    def scores(item, i):
        starts, limits, g = item
        place = lax.broadcasted_iota(jnp.int32, (PIECE, 2 * p), 0)
        bias = jnp.concatenate([jnp.where(place < c, 0.0, NEG) for c in limits], axis=0)
        cols = slice(2 * i * hd, 2 * (i + 1) * hd)
        keys = jnp.concatenate([kv_ref[pl.ds(a, PIECE), cols] for a in starts], axis=0)
        return jnp.dot(keys, qd_ref[g, i], preferred_element_type=jnp.float32) + bias

    def soften(state, i, s):
        tops, sums = state
        old = lanes_of(tops, i)
        top = jnp.maximum(old, jnp.max(s, axis=0, keepdims=True))
        keep = jnp.exp(old - top)
        e = jnp.exp(s - top)
        mass = lanes_of(sums, i) * keep + jnp.sum(e, axis=0, keepdims=True)
        return top, mass, keep, e.astype(jnp.bfloat16)

    def mix(item, i, e):
        vcols = slice(width + 2 * i * hd, width + 2 * (i + 1) * hd)
        values = jnp.concatenate([kv_ref[pl.ds(a, PIECE), vcols] for a in item[0]], axis=0)
        return lax.dot_general(
            values, e, (((0,), (0,)), ((), ())), preferred_element_type=jnp.float32
        )

    def put(item, i, soft, out):
        g = item[2]
        top, mass, keep, _ = soft
        for k in range(2):
            h = 2 * i + k
            lanes = slice(k * p, (k + 1) * p)
            down = slice(h * hd, (h + 1) * hd)
            acc_ref[g, down, :] = acc_ref[g, down, :] * keep[:, lanes] + out[k * hd : (k + 1) * hd, lanes]
            l_ref[g, h : h + 1, :] = mass[:, lanes]
            m_ref[g, h : h + 1, :] = top[:, lanes]

    def finish(item, state, read, ahead):
        last = None
        for i in range(pairs):
            ahead(i)
            soft = soften(state, i, read(i))
            out = mix(item, i, soft[3])
            if last is not None:
                put(item, *last)
            last = (i, soft, out)
        put(item, *last)

    def store(item):
        def ahead(i):
            s_ref[i] = scores(item, i)

        return ahead

    def two(u, carry):
        one, other, after = look(2 * u), look(2 * u + 1), look(2 * u + 2)
        held = {}

        def hold(i):
            held[i] = scores(other, i)

        finish(one, (m_ref[one[2]], l_ref[one[2]]), lambda i: s_ref[i], hold)
        finish(other, (m_ref[other[2]], l_ref[other[2]]), lambda i: held[i], store(after))
        return carry

    first = store(look(0))
    for i in range(pairs):
        first(i)
    lax.fori_loop(0, lax.shift_right_logical(items + 1, 1), two, 0)


def near_kernel(dims, masks_hbm, counts_hbm, normed_ref, pair_ref, w_ref, qd_ref, acc_ref, m_ref,
                l_ref, kv_ref, s_ref, table_ref, owner_ref, masks_ref, counts_ref, sems):
    by, bz, p, width, n = dims
    nb = by * bz
    hd = width // HEADS
    copies = [
        pltpu.make_async_copy(masks_hbm, masks_ref, sems.at[0]),
        pltpu.make_async_copy(counts_hbm, counts_ref, sems.at[1]),
    ]
    for copy in copies:
        copy.start()
    me = lax.axis_index("gx")
    even = me % 2 == 0
    blank = jnp.zeros((hd, p), jnp.bfloat16)
    acc_ref[...] = jnp.zeros_like(acc_ref)
    l_ref[...] = jnp.zeros_like(l_ref)
    m_ref[...] = jnp.full_like(m_ref, NEG)

    def put_q(col, part):
        part = part.astype(jnp.bfloat16) * jnp.bfloat16(1.0 / hd**0.5)
        for g in range(nb):
            turned = part[g * p : (g + 1) * p, :].T
            for h in range(TILE // hd):
                i, k = (col // hd + h) // 2, h % 2
                down = slice(k * hd, (k + 1) * hd)
                qd_ref[g, i, down, k * p : (k + 1) * p] = turned[h * hd : (h + 1) * hd, :]
                qd_ref[g, i, down, (1 - k) * p : (2 - k) * p] = blank

    project(normed_ref, w_ref, 0, width, put_q)
    for copy in copies:
        copy.wait()
    other = jnp.where(even, me + 1, me - 1)
    present = (other >= 0) & (other < n)
    slabs = [(None, me, True), (even, jnp.clip(other, 0, n - 1), present)]
    items = plan(slabs, masks_ref, counts_ref, table_ref, owner_ref, by, bz, p)
    project(normed_ref, w_ref, width, 3 * width, put_keys(kv_ref, 0, width))
    project(pair_ref, w_ref, width, 3 * width, put_keys(kv_ref, nb * p, width))
    work(items, table_ref, owner_ref, kv_ref, qd_ref, s_ref, m_ref, l_ref, acc_ref, width, p)


def far_kernel(dims, masks_hbm, counts_hbm, far_ref, w_ref, w_out_ref, tiled_ref, qd_ref,
               acc_in, m_in, l_in, out_hbm, acc_ref, m_ref, l_ref, attn_ref, out_ref, kv_ref, s_ref,
               table_ref, owner_ref, masks_ref, counts_ref, sems):
    by, bz, p, width, n = dims
    nb = by * bz
    hd = width // HEADS
    copies = [
        pltpu.make_async_copy(masks_hbm, masks_ref, sems.at[0]),
        pltpu.make_async_copy(counts_hbm, counts_ref, sems.at[1]),
    ]
    for copy in copies:
        copy.start()
    me = lax.axis_index("gx")
    even = me % 2 == 0
    project(far_ref, w_ref, width, 2 * width, put_keys(kv_ref, 0, width))
    for copy in copies:
        copy.wait()
    other = jnp.where(even, me - 1, me + 1)
    present = (other >= 0) & (other < n)
    slabs = [(jnp.logical_not(even), jnp.clip(other, 0, n - 1), present)]
    items = plan(slabs, masks_ref, counts_ref, table_ref, owner_ref, by, bz, p)
    project(far_ref, w_ref, 2 * width, 3 * width, put_keys(kv_ref, 0, width))
    work(items, table_ref, owner_ref, kv_ref, qd_ref, s_ref, m_ref, l_ref, acc_ref, width, p)
    row = lax.broadcasted_iota(jnp.int32, (p, width), 0)
    ends = []
    for lo in range(0, nb, 3):
        some = range(lo, min(lo + 3, nb))
        for g in some:
            inverse = 1.0 / l_ref[g]
            parts = [
                (acc_ref[g, h * hd : (h + 1) * hd, :] * inverse[h : h + 1, :]).astype(jnp.bfloat16)
                for h in range(HEADS)
            ]
            attn_ref[g * p : (g + 1) * p, :] = jnp.concatenate(parts, axis=0).T
        mixed = jnp.dot(
            attn_ref[lo * p : (lo + len(some)) * p, :], w_out_ref[...],
            preferred_element_type=jnp.float32,
        )
        for k, g in enumerate(some):
            part = mixed[k * p : (k + 1) * p] + tiled_ref[g].astype(jnp.float32)
            part = jnp.where(row < counts_ref[g // bz, g % bz, me], part, 0.0)
            out_ref[g] = part.astype(jnp.bfloat16)
        held = pl.ds(lo, len(some))
        end = pltpu.make_async_copy(out_ref.at[held], out_hbm.at[held], sems.at[2 + lo // 3])
        end.start()
        ends.append(end)
    for end in ends:
        end.wait()


def shards(points, order, masks, counts, gain, shift_bias, w_qkv, w_out):
    _, by, bz, p, width = points.shape
    n = lax.axis_size("gx")
    nb = by * bz
    dims = (by, bz, p, width, n)
    pairs = [e for i in range(0, n - 1, 2) for e in ((i, i + 1), (i + 1, i))]
    across = [e for i in range(1, n - 1, 2) for e in ((i, i + 1), (i + 1, i))]
    counts = counts.transpose(1, 2, 0)
    pin = lambda value: pltpu.with_memory_space_constraint(value, pltpu.HBM)
    masks, counts = pin(masks), pin(counts)
    shape = jax.ShapeDtypeStruct
    dma = pltpu.SemaphoreType.DMA
    vmem = pl.BlockSpec(memory_space=pltpu.VMEM)
    hbm = pl.BlockSpec(memory_space=pltpu.HBM)
    tiled, normed, w_here, w_out_here = pl.pallas_call(
        functools.partial(norm_kernel, dims),
        name="norm",
        out_shape=[
            shape((nb, p, width), jnp.bfloat16),
            shape((nb * p, width), jnp.bfloat16),
            shape(w_qkv.shape, jnp.bfloat16),
            shape(w_out.shape, jnp.bfloat16),
        ],
        in_specs=[hbm] * 6,
        out_specs=[vmem] * 4,
        scratch_shapes=[
            pltpu.VMEM((nb, p, width), jnp.bfloat16),
            pltpu.VMEM(order.shape, jnp.int32),
            pltpu.VMEM((1, width), jnp.float32),
            pltpu.VMEM((1, width), jnp.float32),
            dma((nb,)),
            dma((5,)),
        ],
        cost_estimate=pl.CostEstimate(
            flops=2 * nb * p * p * width, transcendentals=0, bytes_accessed=2 << 20
        ),
        compiler_params=pltpu.CompilerParams(vmem_limit_bytes=24 << 20),
    )(
        pin(points.reshape(nb, p, width)),
        pin(order),
        pin(gain.reshape(1, width)),
        pin(shift_bias.reshape(1, width)),
        pin(w_qkv),
        pin(w_out),
    )
    far = lax.ppermute(normed, "gx", across)
    pair = lax.ppermute(normed, "gx", pairs)
    slots = len(reach(by, bz))

    def scratch(slabs):
        most = nb * slabs * slots * (p // PIECE) + 4 * SPAN
        return [
            pltpu.VMEM((slabs * nb * p, 2 * width), jnp.bfloat16),
            pltpu.VMEM((HEADS // 2, PIECE * SPAN, 2 * p), jnp.float32),
            pltpu.SMEM((2, most), jnp.int32),
            pltpu.SMEM((most // SPAN,), jnp.int32),
            pltpu.SMEM(masks.shape, jnp.int32),
            pltpu.SMEM(counts.shape, jnp.int32),
        ]

    state = [
        shape((nb, width, p), jnp.float32),
        shape((nb, HEADS, p), jnp.float32),
        shape((nb, HEADS, p), jnp.float32),
    ]
    qd, acc, tops, sums = pl.pallas_call(
        functools.partial(near_kernel, dims),
        name="near",
        out_shape=[shape((nb, HEADS // 2, width // HEADS * 2, 2 * p), jnp.bfloat16)] + state,
        in_specs=[hbm, hbm, vmem, vmem, vmem],
        out_specs=[vmem] * 4,
        scratch_shapes=scratch(2) + [dma((2,))],
        cost_estimate=pl.CostEstimate(
            flops=8 * nb * p * width * 5 * width, transcendentals=0, bytes_accessed=8 << 20
        ),
        compiler_params=pltpu.CompilerParams(vmem_limit_bytes=40 << 20),
    )(masks, counts, normed, pair, w_here)
    out = pl.pallas_call(
        functools.partial(far_kernel, dims),
        name="far",
        out_shape=[shape((nb, p, width), jnp.bfloat16)] + state,
        in_specs=[hbm, hbm] + [vmem] * 8,
        out_specs=[hbm] + [vmem] * 3,
        scratch_shapes=[
            pltpu.VMEM((nb * p, width), jnp.bfloat16),
            pltpu.VMEM((nb, p, width), jnp.bfloat16),
        ]
        + scratch(1)
        + [dma((2 + -(-nb // 3),))],
        input_output_aliases={7: 1, 8: 2, 9: 3},
        cost_estimate=pl.CostEstimate(
            flops=4 * nb * p * width * 3 * width, transcendentals=0, bytes_accessed=8 << 20
        ),
        compiler_params=pltpu.CompilerParams(vmem_limit_bytes=40 << 20),
    )(masks, counts, far, w_here, w_out_here, tiled, qd, acc, tops, sums)[0]
    return out.reshape(points.shape)


def solution(mesh):
    placed = (
        P(("groups", "gx"), None, None, None, None),
        P(("groups", "gx"), None, None, None),
        P(("groups", "gx"), None, None, None),
        P("groups", None, None),
        P(),
        P(),
        P(),
        P(),
    )
    return jax.shard_map(
        shards,
        mesh=mesh,
        in_specs=placed,
        out_specs=P(("groups", "gx"), None, None, None, None),
        check_vma=False,
    )
```

```python
import functools

import jax
import jax.numpy as jnp
from jax import lax
from jax.experimental import pallas as pl
from jax.experimental.pallas import tpu as pltpu
from jax.sharding import PartitionSpec as P

HEADS = 8
TILE = 256
NEG = -1e30
MESH = pl.DeviceIdType.MESH


def column_of(a, b, c):
    index = 9 * (a + 1) + 3 * (b + 1) + (c + 1)
    return index if index < 13 else index - 1


def reach(by, bz):
    spans = [(b, c) for b in (0, -1, 1) for c in (0, -1, 1)]
    return [o for o in spans if (by > 1 or o[0] == 0) and (bz > 1 or o[1] == 0)]


def spot(k, bz):
    return (k, 0) if bz == 1 else (k // bz, k % bz)


def arrange(order_ref, pts_ref, k, bz, gain_ref, shift_ref):
    p = pts_ref.shape[1]
    j, l = spot(k, bz)
    row = order_ref[0, j, pl.ds(l, 1), :]
    pick = lax.broadcasted_iota(jnp.int32, (p, p), 0) == row
    pick = jnp.where(pick, 1.0, 0.0).astype(jnp.bfloat16)
    tiled = lax.dot_general(
        pick, pts_ref[k], (((0,), (0,)), ((), ())), preferred_element_type=jnp.float32
    )
    mean = jnp.mean(tiled, axis=-1, keepdims=True)
    away = tiled - mean
    var = jnp.mean(away * away, axis=-1, keepdims=True)
    normed = away * lax.rsqrt(var + 1e-05) * gain_ref[...] + shift_ref[...]
    return tiled.astype(jnp.bfloat16), normed.astype(jnp.bfloat16)


def project(normed_ref, w_ref, lo, hi, put):
    for col in range(lo, hi, TILE):
        part = jnp.dot(
            normed_ref[...], w_ref[:, col : col + TILE], preferred_element_type=jnp.float32
        )
        put(col, part)


def put_keys(kv_ref, s, width):
    def put(col, part):
        nb, p = kv_ref.shape[1:3]
        part = part.astype(jnp.bfloat16).reshape(nb, p, TILE)
        kv_ref[s, :, :, col - width : col - width + TILE] = part

    return put


def flow(rounds, items, kv_ref, qd_ref, s_ref, limit_ref, m_ref, l_ref, acc_ref, width, p):
    hd = width // HEADS
    pairs = HEADS // 2

    def lanes_of(both, i):
        return jnp.concatenate([both[2 * i : 2 * i + 1], both[2 * i + 1 : 2 * i + 2]], axis=1)

    def scores(item, i):
        s, k, g, at = item
        place = lax.broadcasted_iota(jnp.int32, (p, 2 * p), 0)
        bias = jnp.where(place < limit_ref[at], 0.0, NEG)
        keys = kv_ref[s, k, :, 2 * i * hd : 2 * (i + 1) * hd]
        return jnp.dot(keys, qd_ref[g, i], preferred_element_type=jnp.float32) + bias

    def soften(state, i, s):
        tops, sums = state
        old = lanes_of(tops, i)
        top = jnp.maximum(old, jnp.max(s, axis=0, keepdims=True))
        keep = jnp.exp(old - top)
        e = jnp.exp(s - top)
        mass = lanes_of(sums, i) * keep + jnp.sum(e, axis=0, keepdims=True)
        return top, mass, keep, e.astype(jnp.bfloat16)

    def mix(item, i, e):
        values = kv_ref[item[0], item[1], :, width + 2 * i * hd : width + 2 * (i + 1) * hd]
        return lax.dot_general(
            values, e, (((0,), (0,)), ((), ())), preferred_element_type=jnp.float32
        )

    def put(item, i, soft, out):
        g = item[2]
        top, mass, keep, _ = soft
        for k in range(2):
            h = 2 * i + k
            lanes = slice(k * p, (k + 1) * p)
            down = slice(h * hd, (h + 1) * hd)
            old = acc_ref[g, down, :] * keep[:, lanes]
            acc_ref[g, down, :] = old + out[k * hd : (k + 1) * hd, lanes]
            l_ref[g, h : h + 1, :] = mass[:, lanes]
            m_ref[g, h : h + 1, :] = top[:, lanes]

    def finish(item, read, ahead):
        state = m_ref[item[2]], l_ref[item[2]]
        last = None
        for i in range(pairs):
            ahead(i)
            soft = soften(state, i, read(i))
            out = mix(item, i, soft[3])
            if last is not None:
                put(item, *last)
            last = (i, soft, out)
        put(item, *last)

    def store(item):
        def ahead(i):
            s_ref[i] = scores(item, i)

        return ahead

    def one(u, carry):
        now = items(u)
        after = items((u + 1) % rounds)[0] if rounds > 1 else None
        held = [{} for _ in now]
        for t, item in enumerate(now):
            if t + 1 < len(now):
                ahead = lambda i, t=t: held[t + 1].update({i: scores(now[t + 1], i)})
            elif after is not None:
                ahead = store(after)
            else:
                ahead = lambda i: None
            read = (lambda i: s_ref[i]) if t == 0 else (lambda i, t=t: held[t][i])
            finish(item, read, ahead)
        return carry

    first = store(items(0)[0])
    for i in range(pairs):
        first(i)
    if rounds > 1:
        lax.fori_loop(0, rounds, one, 0)
    else:
        one(0, 0)


def main_kernel(dims, pts_hbm, order_hbm, masks_hbm, counts_hbm, gain_hbm, shift_hbm, w_hbm,
                w_out_hbm, tiled_ref, acc_ref, l_ref, live_ref, w_out_ref, pts_ref, order_ref,
                normed_ref, block_ref, kv_ref, qd_ref, s_ref, m_ref, gain_ref, shift_ref, w_ref, limit_ref,
                masks_ref, counts_ref, sems, own_sem, pair_send, pair_recv, far_send, far_recv):
    by, bz, p, width, n = dims
    nb = by * bz
    hd = width // HEADS
    me = lax.axis_index("gx")
    odd = me % 2
    pair = me + 1 - 2 * odd
    far = me - 1 + 2 * odd
    has = (far >= 0) & (far < n)
    barrier = pltpu.get_barrier_semaphore()
    pl.semaphore_signal(barrier, inc=1, device_id={"gx": pair}, device_id_type=MESH)

    @pl.when(has)
    def _():
        pl.semaphore_signal(barrier, inc=1, device_id={"gx": far}, device_id_type=MESH)

    small = [
        pltpu.make_async_copy(order_hbm, order_ref.at[0], sems.at[0]),
        pltpu.make_async_copy(gain_hbm, gain_ref, sems.at[1]),
        pltpu.make_async_copy(shift_hbm, shift_ref, sems.at[2]),
        pltpu.make_async_copy(masks_hbm, masks_ref, sems.at[3]),
        pltpu.make_async_copy(counts_hbm, counts_ref, sems.at[4]),
    ]
    own = pltpu.make_async_copy(pts_hbm, pts_ref.at[0], own_sem)
    weights = pltpu.make_async_copy(w_hbm, w_ref, sems.at[5])
    weights_out = pltpu.make_async_copy(w_out_hbm, w_out_ref, sems.at[6])
    for copy in small + [own, weights, weights_out]:
        copy.start()

    def send(source, target, out_sem, in_sem, device):
        return pltpu.make_async_remote_copy(
            src_ref=source, dst_ref=target, send_sem=out_sem, recv_sem=in_sem,
            device_id={"gx": device}, device_id_type=MESH,
        )

    def far_block(k):
        return send(pts_hbm.at[k], pts_ref.at[2, k], far_send.at[k], far_recv.at[k], far)

    far_order = send(order_hbm, order_ref.at[2], far_send.at[nb], far_recv.at[nb], far)
    pair_order = send(order_hbm, order_ref.at[1], pair_send.at[0], pair_recv.at[0], pair)
    pair_points = send(pts_hbm, pts_ref.at[1], pair_send.at[1], pair_recv.at[1], pair)

    @pl.when(has)
    def _():
        pl.semaphore_wait(barrier, 2)

    @pl.when(jnp.logical_not(has))
    def _():
        pl.semaphore_wait(barrier, 1)

    @pl.when(has)
    def _():
        far_order.start()
        for k in range(nb):
            far_block(k).start()

    pair_order.start()
    pair_points.start()

    for copy in small:
        copy.wait()
    near = reach(by, bz)
    reachable = len(near)
    here = has.astype(jnp.int32)
    slabs = [(me, 0, 1), (pair, 1 - 2 * odd, 1), ((far + n) % n, 2 * odd - 1, here)]
    for s, (at, _, there) in enumerate(slabs):
        for g in range(nb):
            j, l = spot(g, bz)
            for r, (b, c) in enumerate(near):
                inside = 0 <= j + b < by and 0 <= l + c < bz
                k = g + b * bz + c
                key = g if s < 2 else k % nb
                slot = (s * nb + key) * reachable + r
                if not inside:
                    limit_ref[slot] = 0
                    continue
                count = counts_ref[j + b, l + c, at] * there
                if s == 0 and (b, c) != (0, 0):
                    count = count * masks_ref[0, j, l, column_of(0, b, c)]
                if s > 0:
                    plus, minus = column_of(1, b, c), column_of(-1, b, c)
                    sign = 1 - odd if s == 1 else odd
                    count = count * masks_ref[0, j, l, minus + (plus - minus) * sign]
                limit_ref[slot] = count
    for g in range(nb):
        j, l = spot(g, bz)
        live_ref[g] = jnp.full(live_ref.shape[1:], counts_ref[j, l, me], jnp.int32)
    acc_ref[...] = jnp.zeros_like(acc_ref)
    l_ref[...] = jnp.zeros_like(l_ref)
    m_ref[...] = jnp.full_like(m_ref, NEG)

    own.wait()
    for g in range(nb):
        tiled, normed = arrange(order_ref.at[0], pts_ref.at[0], g, bz, gain_ref, shift_ref)
        tiled_ref[g] = tiled
        normed_ref[g * p : (g + 1) * p, :] = normed
    weights.wait()
    weights_out.wait()
    blank = jnp.zeros((hd, p), jnp.bfloat16)

    def put_q(col, part):
        part = part.astype(jnp.bfloat16) * jnp.bfloat16(1.0 / hd**0.5)
        for g in range(nb):
            turned = part[g * p : (g + 1) * p, :].T
            for h in range(TILE // hd):
                i, k = (col // hd + h) // 2, h % 2
                down = slice(k * hd, (k + 1) * hd)
                qd_ref[g, i, down, k * p : (k + 1) * p] = turned[h * hd : (h + 1) * hd, :]
                qd_ref[g, i, down, (1 - k) * p : (2 - k) * p] = blank

    project(normed_ref, w_ref, 0, width, put_q)
    project(normed_ref, w_ref, width, 3 * width, put_keys(kv_ref, 0, width))
    rest = (kv_ref, qd_ref, s_ref, limit_ref, m_ref, l_ref, acc_ref, width, p)

    def around(s):
        def items(g):
            return [
                (s, (g + b * bz + c + nb) % nb, g, (s * nb + g) * reachable + r)
                for r, (b, c) in enumerate(near)
            ]

        return items

    flow(nb, around(0), *rest)
    pair_order.wait_recv()
    pair_points.wait_recv()
    for g in range(nb):
        _, normed = arrange(order_ref.at[1], pts_ref.at[1], g, bz, gain_ref, shift_ref)
        normed_ref[g * p : (g + 1) * p, :] = normed
    project(normed_ref, w_ref, width, 3 * width, put_keys(kv_ref, 1, width))
    flow(nb, around(1), *rest)

    @pl.when(has)
    def _():
        far_order.wait_recv()

        def block(k, carry):
            far_block(k).wait_recv()
            _, normed = arrange(order_ref.at[2], pts_ref.at[2], k, bz, gain_ref, shift_ref)
            block_ref[...] = normed
            for col in range(width, 3 * width, TILE):
                part = jnp.dot(
                    block_ref[...], w_ref[:, col : col + TILE], preferred_element_type=jnp.float32
                )
                kv_ref[2, k, :, col - width : col - width + TILE] = part.astype(jnp.bfloat16)

            def items(u):
                return [
                    (2, k, (k - b * bz - c + nb) % nb, (2 * nb + k) * reachable + r)
                    for r, (b, c) in enumerate(near)
                ]

            flow(1, items, *rest)
            return carry

        lax.fori_loop(0, nb, block, 0)
        far_order.wait_send()
        for k in range(nb):
            far_block(k).wait_send()

    pair_order.wait_send()
    pair_points.wait_send()


def tail_kernel(dims, acc_ref, l_ref, tiled_ref, live_ref, w_out_ref, out_hbm, attn_ref, out_ref, sems):
    by, bz, p, width, n = dims
    nb = by * bz
    hd = width // HEADS
    row = lax.broadcasted_iota(jnp.int32, (p, width), 0)
    ends = []
    for lo in range(0, nb, 3):
        some = range(lo, min(lo + 3, nb))
        for g in some:
            inverse = 1.0 / l_ref[g]
            parts = [
                (acc_ref[g, h * hd : (h + 1) * hd, :] * inverse[h : h + 1, :]).astype(jnp.bfloat16)
                for h in range(HEADS)
            ]
            attn_ref[g * p : (g + 1) * p, :] = jnp.concatenate(parts, axis=0).T
        mixed = jnp.dot(
            attn_ref[lo * p : (lo + len(some)) * p, :], w_out_ref[...],
            preferred_element_type=jnp.float32,
        )
        for k, g in enumerate(some):
            part = mixed[k * p : (k + 1) * p] + tiled_ref[g].astype(jnp.float32)
            part = jnp.where(row < live_ref[g, :1, :], part, 0.0)
            out_ref[g] = part.astype(jnp.bfloat16)
        held = pl.ds(lo, len(some))
        end = pltpu.make_async_copy(out_ref.at[held], out_hbm.at[held], sems.at[lo // 3])
        end.start()
        ends.append(end)
    for end in ends:
        end.wait()


def shards(points, order, masks, counts, gain, shift_bias, w_qkv, w_out):
    _, by, bz, p, width = points.shape
    n = lax.axis_size("gx")
    nb = by * bz
    dims = (by, bz, p, width, n)
    counts = counts.transpose(1, 2, 0)
    pin = lambda value: pltpu.with_memory_space_constraint(value, pltpu.HBM)
    shape = jax.ShapeDtypeStruct
    dma = pltpu.SemaphoreType.DMA
    vmem = pl.BlockSpec(memory_space=pltpu.VMEM)
    hbm = pl.BlockSpec(memory_space=pltpu.HBM)
    half = jnp.bfloat16
    tiled, acc, sums, live, w_here = pl.pallas_call(
        functools.partial(main_kernel, dims),
        name="main",
        out_shape=[
            shape((nb, p, width), half),
            shape((nb, width, p), jnp.float32),
            shape((nb, HEADS, p), jnp.float32),
            shape((nb, 8, width), jnp.int32),
            shape(w_out.shape, half),
        ],
        in_specs=[hbm] * 8,
        out_specs=[vmem] * 5,
        scratch_shapes=[
            pltpu.VMEM((3, nb, p, width), half),
            pltpu.VMEM((3,) + order.shape, jnp.int32),
            pltpu.VMEM((nb * p, width), half),
            pltpu.VMEM((p, width), half),
            pltpu.VMEM((3, nb, p, 2 * width), half),
            pltpu.VMEM((nb, HEADS // 2, width // HEADS * 2, 2 * p), half),
            pltpu.VMEM((HEADS // 2, p, 2 * p), jnp.float32),
            pltpu.VMEM((nb, HEADS, p), jnp.float32),
            pltpu.VMEM((1, width), jnp.float32),
            pltpu.VMEM((1, width), jnp.float32),
            pltpu.VMEM(w_qkv.shape, half),
            pltpu.SMEM((3 * nb * len(reach(by, bz)),), jnp.int32),
            pltpu.SMEM(masks.shape, jnp.int32),
            pltpu.SMEM(counts.shape, jnp.int32),
            dma((7,)),
            dma,
            dma((2,)),
            dma((2,)),
            dma((nb + 1,)),
            dma((nb + 1,)),
        ],
        cost_estimate=pl.CostEstimate(
            flops=2 * nb * p * width * 24 * width, transcendentals=0, bytes_accessed=8 << 20
        ),
        compiler_params=pltpu.CompilerParams(
            vmem_limit_bytes=48 << 20, collective_id=0, has_side_effects=True
        ),
    )(
        pin(points.reshape(nb, p, width)),
        pin(order),
        pin(masks),
        pin(counts),
        pin(gain.reshape(1, width)),
        pin(shift_bias.reshape(1, width)),
        pin(w_qkv),
        pin(w_out),
    )
    out = pl.pallas_call(
        functools.partial(tail_kernel, dims),
        name="tail",
        out_shape=shape((nb, p, width), half),
        in_specs=[vmem] * 5,
        out_specs=hbm,
        scratch_shapes=[
            pltpu.VMEM((nb * p, width), half),
            pltpu.VMEM((nb, p, width), half),
            dma((-(-nb // 3),)),
        ],
        cost_estimate=pl.CostEstimate(
            flops=2 * nb * p * width * width, transcendentals=0, bytes_accessed=2 << 20
        ),
        compiler_params=pltpu.CompilerParams(vmem_limit_bytes=16 << 20),
    )(acc, sums, tiled, live, w_here)
    return out.reshape(points.shape)


def solution(mesh):
    placed = (
        P(("groups", "gx"), None, None, None, None),
        P(("groups", "gx"), None, None, None),
        P(("groups", "gx"), None, None, None),
        P("groups", None, None),
        P(),
        P(),
        P(),
        P(),
    )
    return jax.shard_map(
        shards,
        mesh=mesh,
        in_specs=placed,
        out_specs=P(("groups", "gx"), None, None, None, None),
        check_vma=False,
    )
```

```python
import functools

import jax
import jax.numpy as jnp
from jax import lax
from jax.experimental import pallas as pl
from jax.experimental.pallas import tpu as pltpu
from jax.sharding import PartitionSpec as P

HEADS = 8
TILE = 256
NEG = -1e30
MESH = pl.DeviceIdType.MESH


def column_of(a, b, c):
    index = 9 * (a + 1) + 3 * (b + 1) + (c + 1)
    return index if index < 13 else index - 1


def reach(by, bz):
    spans = [(b, c) for b in (-1, 0, 1) for c in (-1, 0, 1)]
    return [o for o in spans if (by > 1 or o[0] == 0) and (bz > 1 or o[1] == 0)]


def links(by, bz, k, side):
    nb = by * bz
    found = []
    for r, (b, c) in enumerate(reach(by, bz)):
        if isinstance(k, int):
            j, l = k // bz + side * b, k % bz + side * c
            if not (0 <= j < by and 0 <= l < bz):
                continue
        other = (k + side * (b * bz + c) + nb) % nb
        found.append((r, k, other))
    return found


def spot(k, bz):
    return (k, 0) if bz == 1 else (k // bz, k % bz)


def arrange(order_ref, pts_ref, k, bz, gain_ref, shift_ref):
    p = pts_ref.shape[1]
    j, l = spot(k, bz)
    row = order_ref[0, j, pl.ds(l, 1), :]
    pick = lax.broadcasted_iota(jnp.int32, (p, p), 0) == row
    pick = jnp.where(pick, 1.0, 0.0).astype(jnp.bfloat16)
    tiled = lax.dot_general(
        pick, pts_ref[k], (((0,), (0,)), ((), ())), preferred_element_type=jnp.float32
    )
    mean = jnp.mean(tiled, axis=-1, keepdims=True)
    away = tiled - mean
    var = jnp.mean(away * away, axis=-1, keepdims=True)
    normed = away * lax.rsqrt(var + 1e-05) * gain_ref[...] + shift_ref[...]
    return tiled.astype(jnp.bfloat16), normed.astype(jnp.bfloat16)


def project(normed_ref, w_ref, lo, hi, put):
    for col in range(lo, hi, TILE):
        part = jnp.dot(
            normed_ref[...], w_ref[:, col : col + TILE], preferred_element_type=jnp.float32
        )
        put(col, part)


def put_keys(kv_ref, s, width):
    def put(col, part):
        nb, p = kv_ref.shape[1:3]
        part = part.astype(jnp.bfloat16).reshape(nb, p, TILE)
        kv_ref[s, :, :, col - width : col - width + TILE] = part

    return put


def flow(rounds, items, kv_ref, qd_ref, s_ref, limit_ref, m_ref, l_ref, acc_ref, width, p):
    hd = width // HEADS
    pairs = HEADS // 2

    def lanes_of(both, i):
        return jnp.concatenate([both[2 * i : 2 * i + 1], both[2 * i + 1 : 2 * i + 2]], axis=1)

    def scores(item, i):
        s, k, g, at = item
        place = lax.broadcasted_iota(jnp.int32, (p, 2 * p), 0)
        bias = jnp.where(place < limit_ref[at], 0.0, NEG)
        keys = kv_ref[s, k, :, 2 * i * hd : 2 * (i + 1) * hd]
        return jnp.dot(keys, qd_ref[g, i], preferred_element_type=jnp.float32) + bias

    def soften(state, i, s):
        tops, sums = state
        old = lanes_of(tops, i)
        top = jnp.maximum(old, jnp.max(s, axis=0, keepdims=True))
        keep = jnp.exp(old - top)
        e = jnp.exp(s - top)
        mass = lanes_of(sums, i) * keep + jnp.sum(e, axis=0, keepdims=True)
        return top, mass, keep, e.astype(jnp.bfloat16)

    def mix(item, i, e):
        values = kv_ref[item[0], item[1], :, width + 2 * i * hd : width + 2 * (i + 1) * hd]
        return lax.dot_general(
            values, e, (((0,), (0,)), ((), ())), preferred_element_type=jnp.float32
        )

    def put(item, i, soft, out):
        g = item[2]
        top, mass, keep, _ = soft
        for k in range(2):
            h = 2 * i + k
            lanes = slice(k * p, (k + 1) * p)
            down = slice(h * hd, (h + 1) * hd)
            old = acc_ref[g, down, :] * keep[:, lanes]
            acc_ref[g, down, :] = old + out[k * hd : (k + 1) * hd, lanes]
            l_ref[g, h : h + 1, :] = mass[:, lanes]
            m_ref[g, h : h + 1, :] = top[:, lanes]

    def finish(item, read, ahead):
        state = m_ref[item[2]], l_ref[item[2]]
        last = None
        for i in range(pairs):
            ahead(i)
            soft = soften(state, i, read(i))
            out = mix(item, i, soft[3])
            if last is not None:
                put(item, *last)
            last = (i, soft, out)
        put(item, *last)

    def store(item):
        def ahead(i):
            s_ref[i] = scores(item, i)

        return ahead

    def one(u, carry):
        now = items(u)
        after = items((u + 1) % rounds)[0] if rounds > 1 else None
        held = [{} for _ in now]
        for t, item in enumerate(now):
            if t + 1 < len(now):
                ahead = lambda i, t=t: held[t + 1].update({i: scores(now[t + 1], i)})
            elif after is not None:
                ahead = store(after)
            else:
                ahead = lambda i: None
            read = (lambda i: s_ref[i]) if t == 0 else (lambda i, t=t: held[t][i])
            finish(item, read, ahead)
        return carry

    first = store(items(0)[0])
    for i in range(pairs):
        first(i)
    if rounds > 1:
        lax.fori_loop(0, rounds, one, 0)
    else:
        one(0, 0)


def main_kernel(dims, pts_hbm, order_hbm, masks_hbm, counts_hbm, gain_hbm, shift_hbm, w_hbm,
                w_out_hbm, tiled_ref, acc_ref, l_ref, live_ref, w_out_ref, pts_ref, order_ref,
                normed_ref, block_ref, kv_ref, qd_ref, s_ref, m_ref, gain_ref, shift_ref, w_ref, limit_ref,
                masks_ref, counts_ref, sems, own_sem, pair_send, pair_recv, far_send, far_recv):
    by, bz, p, width, n = dims
    nb = by * bz
    hd = width // HEADS
    me = lax.axis_index("gx")
    odd = me % 2
    pair = me + 1 - 2 * odd
    far = me - 1 + 2 * odd
    has = (far >= 0) & (far < n)
    barrier = pltpu.get_barrier_semaphore()
    pl.semaphore_signal(barrier, inc=1, device_id={"gx": pair}, device_id_type=MESH)

    @pl.when(has)
    def _():
        pl.semaphore_signal(barrier, inc=1, device_id={"gx": far}, device_id_type=MESH)

    small = [
        pltpu.make_async_copy(order_hbm, order_ref.at[0], sems.at[0]),
        pltpu.make_async_copy(gain_hbm, gain_ref, sems.at[1]),
        pltpu.make_async_copy(shift_hbm, shift_ref, sems.at[2]),
        pltpu.make_async_copy(masks_hbm, masks_ref, sems.at[3]),
        pltpu.make_async_copy(counts_hbm, counts_ref, sems.at[4]),
    ]
    own = pltpu.make_async_copy(pts_hbm, pts_ref.at[0], own_sem)
    weights = pltpu.make_async_copy(w_hbm, w_ref, sems.at[5])
    weights_out = pltpu.make_async_copy(w_out_hbm, w_out_ref, sems.at[6])
    for copy in small + [own, weights, weights_out]:
        copy.start()

    def send(source, target, out_sem, in_sem, device):
        return pltpu.make_async_remote_copy(
            src_ref=source, dst_ref=target, send_sem=out_sem, recv_sem=in_sem,
            device_id={"gx": device}, device_id_type=MESH,
        )

    def far_block(k):
        return send(pts_hbm.at[k], pts_ref.at[2, k], far_send.at[k], far_recv.at[k], far)

    far_order = send(order_hbm, order_ref.at[2], far_send.at[nb], far_recv.at[nb], far)
    pair_order = send(order_hbm, order_ref.at[1], pair_send.at[0], pair_recv.at[0], pair)
    pair_points = send(pts_hbm, pts_ref.at[1], pair_send.at[1], pair_recv.at[1], pair)

    @pl.when(has)
    def _():
        pl.semaphore_wait(barrier, 2)

    @pl.when(jnp.logical_not(has))
    def _():
        pl.semaphore_wait(barrier, 1)

    @pl.when(has)
    def _():
        far_order.start()
        for k in range(nb):
            far_block(k).start()

    pair_order.start()
    pair_points.start()

    for copy in small:
        copy.wait()
    near = reach(by, bz)
    reachable = len(near)
    here = has.astype(jnp.int32)
    slabs = [(me, 0, 1), (pair, 1 - 2 * odd, 1), ((far + n) % n, 2 * odd - 1, here)]
    for s, (at, _, there) in enumerate(slabs):
        for g in range(nb):
            j, l = spot(g, bz)
            for r, (b, c) in enumerate(near):
                inside = 0 <= j + b < by and 0 <= l + c < bz
                k = g + b * bz + c
                key = g if s < 2 else k % nb
                slot = (s * nb + key) * reachable + r
                if not inside:
                    limit_ref[slot] = 0
                    continue
                count = counts_ref[j + b, l + c, at] * there
                if s == 0 and (b, c) != (0, 0):
                    count = count * masks_ref[0, j, l, column_of(0, b, c)]
                if s > 0:
                    plus, minus = column_of(1, b, c), column_of(-1, b, c)
                    sign = 1 - odd if s == 1 else odd
                    count = count * masks_ref[0, j, l, minus + (plus - minus) * sign]
                limit_ref[slot] = count
    for g in range(nb):
        j, l = spot(g, bz)
        live_ref[g] = jnp.full(live_ref.shape[1:], counts_ref[j, l, me], jnp.int32)
    acc_ref[...] = jnp.zeros_like(acc_ref)
    l_ref[...] = jnp.zeros_like(l_ref)
    m_ref[...] = jnp.full_like(m_ref, NEG)

    own.wait()
    for g in range(nb):
        tiled, normed = arrange(order_ref.at[0], pts_ref.at[0], g, bz, gain_ref, shift_ref)
        tiled_ref[g] = tiled
        normed_ref[g * p : (g + 1) * p, :] = normed
    weights.wait()
    weights_out.wait()
    blank = jnp.zeros((hd, p), jnp.bfloat16)

    def put_q(col, part):
        part = part.astype(jnp.bfloat16) * jnp.bfloat16(1.0 / hd**0.5)
        for g in range(nb):
            turned = part[g * p : (g + 1) * p, :].T
            for h in range(TILE // hd):
                i, k = (col // hd + h) // 2, h % 2
                down = slice(k * hd, (k + 1) * hd)
                qd_ref[g, i, down, k * p : (k + 1) * p] = turned[h * hd : (h + 1) * hd, :]
                qd_ref[g, i, down, (1 - k) * p : (2 - k) * p] = blank

    project(normed_ref, w_ref, 0, width, put_q)
    project(normed_ref, w_ref, width, 3 * width, put_keys(kv_ref, 0, width))
    rest = (kv_ref, qd_ref, s_ref, limit_ref, m_ref, l_ref, acc_ref, width, p)

    def around(s):
        def items(g):
            return [(s, k, g, (s * nb + g) * reachable + r) for r, g, k in links(by, bz, g, 1)]

        def row(u):
            places = [u * per + t + 1 for t in range(per)]
            return [(s, v // 3 + v % 3 - 1, v // 3, s * nb * 3 + v) for v in places]

        if bz > 1 or by == 1:
            return nb, items
        per = max(d for d in (1, 2, 4) if (3 * nb - 2) % d == 0)
        return (3 * nb - 2) // per, row

    flow(*around(0), *rest)
    pair_order.wait_recv()
    pair_points.wait_recv()
    for g in range(nb):
        _, normed = arrange(order_ref.at[1], pts_ref.at[1], g, bz, gain_ref, shift_ref)
        normed_ref[g * p : (g + 1) * p, :] = normed
    project(normed_ref, w_ref, width, 3 * width, put_keys(kv_ref, 1, width))
    flow(*around(1), *rest)

    def fetch(k, between):
        far_block(k).wait_recv()
        _, normed = arrange(order_ref.at[2], pts_ref.at[2], k, bz, gain_ref, shift_ref)
        block_ref[...] = normed
        between()
        for col in range(width, 3 * width, TILE):
            part = jnp.dot(
                block_ref[...], w_ref[:, col : col + TILE], preferred_element_type=jnp.float32
            )
            kv_ref[2, k, :, col - width : col - width + TILE] = part.astype(jnp.bfloat16)

    def served(k):
        def items(u):
            return [(2, k, g, (2 * nb + k) * reachable + r) for r, k, g in links(by, bz, k, -1)]

        flow(1, items, *rest)

    @pl.when(has)
    def _():
        far_order.wait_recv()
        fetch(0, lambda: None)
        if nb > 1:
            fetch(1, lambda: served(0))

        def step(k, carry):
            fetch(k, lambda: served(k - 1))
            return carry

        lax.fori_loop(2, nb, step, 0)
        served(nb - 1)
        far_order.wait_send()
        for k in range(nb):
            far_block(k).wait_send()

    pair_order.wait_send()
    pair_points.wait_send()


def tail_kernel(dims, acc_ref, l_ref, tiled_ref, live_ref, w_out_ref, out_hbm, attn_ref, out_ref, sems):
    by, bz, p, width, n = dims
    nb = by * bz
    hd = width // HEADS
    row = lax.broadcasted_iota(jnp.int32, (p, width), 0)
    ends = []
    for lo in range(0, nb, 3):
        some = range(lo, min(lo + 3, nb))
        for g in some:
            inverse = 1.0 / l_ref[g]
            parts = [
                (acc_ref[g, h * hd : (h + 1) * hd, :] * inverse[h : h + 1, :]).astype(jnp.bfloat16)
                for h in range(HEADS)
            ]
            attn_ref[g * p : (g + 1) * p, :] = jnp.concatenate(parts, axis=0).T
        mixed = jnp.dot(
            attn_ref[lo * p : (lo + len(some)) * p, :], w_out_ref[...],
            preferred_element_type=jnp.float32,
        )
        for k, g in enumerate(some):
            part = mixed[k * p : (k + 1) * p] + tiled_ref[g].astype(jnp.float32)
            part = jnp.where(row < live_ref[g, :1, :], part, 0.0)
            out_ref[g] = part.astype(jnp.bfloat16)
        held = pl.ds(lo, len(some))
        end = pltpu.make_async_copy(out_ref.at[held], out_hbm.at[held], sems.at[lo // 3])
        end.start()
        ends.append(end)
    for end in ends:
        end.wait()


def shards(points, order, masks, counts, gain, shift_bias, w_qkv, w_out):
    _, by, bz, p, width = points.shape
    n = lax.axis_size("gx")
    nb = by * bz
    dims = (by, bz, p, width, n)
    counts = counts.transpose(1, 2, 0)
    pin = lambda value: pltpu.with_memory_space_constraint(value, pltpu.HBM)
    shape = jax.ShapeDtypeStruct
    dma = pltpu.SemaphoreType.DMA
    vmem = pl.BlockSpec(memory_space=pltpu.VMEM)
    hbm = pl.BlockSpec(memory_space=pltpu.HBM)
    half = jnp.bfloat16
    tiled, acc, sums, live, w_here = pl.pallas_call(
        functools.partial(main_kernel, dims),
        name="main",
        out_shape=[
            shape((nb, p, width), half),
            shape((nb, width, p), jnp.float32),
            shape((nb, HEADS, p), jnp.float32),
            shape((nb, 8, width), jnp.int32),
            shape(w_out.shape, half),
        ],
        in_specs=[hbm] * 8,
        out_specs=[vmem] * 5,
        scratch_shapes=[
            pltpu.VMEM((3, nb, p, width), half),
            pltpu.VMEM((3,) + order.shape, jnp.int32),
            pltpu.VMEM((nb * p, width), half),
            pltpu.VMEM((p, width), half),
            pltpu.VMEM((3, nb, p, 2 * width), half),
            pltpu.VMEM((nb, HEADS // 2, width // HEADS * 2, 2 * p), half),
            pltpu.VMEM((HEADS // 2, p, 2 * p), jnp.float32),
            pltpu.VMEM((nb, HEADS, p), jnp.float32),
            pltpu.VMEM((1, width), jnp.float32),
            pltpu.VMEM((1, width), jnp.float32),
            pltpu.VMEM(w_qkv.shape, half),
            pltpu.SMEM((3 * nb * len(reach(by, bz)),), jnp.int32),
            pltpu.SMEM(masks.shape, jnp.int32),
            pltpu.SMEM(counts.shape, jnp.int32),
            dma((7,)),
            dma,
            dma((2,)),
            dma((2,)),
            dma((nb + 1,)),
            dma((nb + 1,)),
        ],
        cost_estimate=pl.CostEstimate(
            flops=2 * nb * p * width * 24 * width, transcendentals=0, bytes_accessed=8 << 20
        ),
        compiler_params=pltpu.CompilerParams(
            vmem_limit_bytes=48 << 20, collective_id=0, has_side_effects=True
        ),
    )(
        pin(points.reshape(nb, p, width)),
        pin(order),
        pin(masks),
        pin(counts),
        pin(gain.reshape(1, width)),
        pin(shift_bias.reshape(1, width)),
        pin(w_qkv),
        pin(w_out),
    )
    out = pl.pallas_call(
        functools.partial(tail_kernel, dims),
        name="tail",
        out_shape=shape((nb, p, width), half),
        in_specs=[vmem] * 5,
        out_specs=hbm,
        scratch_shapes=[
            pltpu.VMEM((nb * p, width), half),
            pltpu.VMEM((nb, p, width), half),
            dma((-(-nb // 3),)),
        ],
        cost_estimate=pl.CostEstimate(
            flops=2 * nb * p * width * width, transcendentals=0, bytes_accessed=2 << 20
        ),
        compiler_params=pltpu.CompilerParams(vmem_limit_bytes=16 << 20),
    )(acc, sums, tiled, live, w_here)
    return out.reshape(points.shape)


def solution(mesh):
    placed = (
        P(("groups", "gx"), None, None, None, None),
        P(("groups", "gx"), None, None, None),
        P(("groups", "gx"), None, None, None),
        P("groups", None, None),
        P(),
        P(),
        P(),
        P(),
    )
    return jax.shard_map(
        shards,
        mesh=mesh,
        in_specs=placed,
        out_specs=P(("groups", "gx"), None, None, None, None),
        check_vma=False,
    )
```

```python
import functools

import jax
import jax.numpy as jnp
from jax import lax
from jax.experimental import pallas as pl
from jax.experimental.pallas import tpu as pltpu
from jax.sharding import PartitionSpec as P

HEADS = 8
TILE = 256
NEG = -1e30
OFF = -3e30
ONES = 16
MESH = pl.DeviceIdType.MESH


def column_of(a, b, c):
    index = 9 * (a + 1) + 3 * (b + 1) + (c + 1)
    return index if index < 13 else index - 1


def reach(by, bz):
    spans = [(b, c) for b in (-1, 0, 1) for c in (-1, 0, 1)]
    return [o for o in spans if (by > 1 or o[0] == 0) and (bz > 1 or o[1] == 0)]


def links(by, bz, k, side):
    nb = by * bz
    found = []
    for r, (b, c) in enumerate(reach(by, bz)):
        if isinstance(k, int):
            j, l = k // bz + side * b, k % bz + side * c
            if not (0 <= j < by and 0 <= l < bz):
                continue
        other = (k + side * (b * bz + c) + nb) % nb
        found.append((r, k, other))
    return found


def spot(k, bz):
    return (k, 0) if bz == 1 else (k // bz, k % bz)


def chosen(order_ref, k, bz, p):
    j, l = spot(k, bz)
    row = order_ref[0, j, pl.ds(l, 1), :]
    pick = lax.broadcasted_iota(jnp.int32, (p, p), 0) == row
    return jnp.where(pick, 1.0, 0.0).astype(jnp.bfloat16)


def norm(values, gain_ref, shift_ref):
    values = values.astype(jnp.float32)
    mean = jnp.mean(values, axis=-1, keepdims=True)
    away = values - mean
    var = jnp.mean(away * away, axis=-1, keepdims=True)
    normed = away * lax.rsqrt(var + 1e-05) * gain_ref[...] + shift_ref[...]
    return normed.astype(jnp.bfloat16)


def project(normed_ref, w_ref, lo, hi, put):
    for col in range(lo, hi, TILE):
        part = jnp.dot(
            normed_ref[...], w_ref[:, col : col + TILE], preferred_element_type=jnp.float32
        )
        put(col, part)


def put_keys(kv_ref, s, width):
    def put(col, part):
        nb, p = kv_ref.shape[1:3]
        part = part.astype(jnp.bfloat16).reshape(nb, p, TILE)
        kv_ref[s, :, :, col - width : col - width + TILE] = part

    return put


def flow(rounds, items, kv_ref, pick_ref, qd_ref, tag_ref, s_ref, on_ref, m_ref, l_ref, acc_ref, width, p):
    hd = width // HEADS
    pairs = HEADS // 2

    def lanes_of(both, i):
        return jnp.concatenate([both[2 * i : 2 * i + 1], both[2 * i + 1 : 2 * i + 2]], axis=1)

    def scores(item, i):
        s, k, g, at = item
        keys = jnp.concatenate(
            [kv_ref[s, k, :, 2 * i * hd : 2 * (i + 1) * hd], pick_ref[s, k]], axis=1
        )
        asked = jnp.concatenate([qd_ref[g, i], tag_ref[s, k]], axis=0)
        return jnp.dot(keys, asked, preferred_element_type=jnp.float32)

    def soften(item, state, i, s):
        off = jnp.where(on_ref[item[3]] == 1, 0.0, OFF)
        old = lanes_of(state, i)
        top = jnp.maximum(old, jnp.max(s, axis=0, keepdims=True) + off)
        keep = jnp.exp(old - top)
        e = jnp.exp(s - (top - off))
        return top, keep, e.astype(jnp.bfloat16)

    def mix(item, i, e):
        values = kv_ref[item[0], item[1], :, width + 2 * i * hd : width + 2 * (i + 1) * hd]
        lines = jnp.concatenate([values.T, jnp.ones((ONES, p), jnp.bfloat16)], axis=0)
        return jnp.dot(lines, e, preferred_element_type=jnp.float32)

    def put(item, i, soft, out):
        g = item[2]
        top, keep, _ = soft
        mass = out[2 * hd : 2 * hd + 1, :]
        for k in range(2):
            h = 2 * i + k
            lanes = slice(k * p, (k + 1) * p)
            down = slice(h * hd, (h + 1) * hd)
            old = acc_ref[g, down, :] * keep[:, lanes]
            acc_ref[g, down, :] = old + out[k * hd : (k + 1) * hd, lanes]
            l_ref[g, h : h + 1, :] = l_ref[g, h : h + 1, :] * keep[:, lanes] + mass[:, lanes]
            m_ref[g, h : h + 1, :] = top[:, lanes]

    def finish(item, read, ahead):
        state = m_ref[item[2]]
        last = None
        for i in range(pairs):
            ahead(i)
            soft = soften(item, state, i, read(i))
            out = mix(item, i, soft[2])
            if last is not None:
                put(item, *last)
            last = (i, soft, out)
        put(item, *last)

    def store(item):
        def ahead(i):
            s_ref[i] = scores(item, i)

        return ahead

    def one(u, carry):
        now = items(u)
        after = items((u + 1) % rounds)[0] if rounds > 1 else None
        held = [{} for _ in now]
        for t, item in enumerate(now):
            if t + 1 < len(now):
                ahead = lambda i, t=t: held[t + 1].update({i: scores(now[t + 1], i)})
            elif after is not None:
                ahead = store(after)
            else:
                ahead = lambda i: None
            read = (lambda i: s_ref[i]) if t == 0 else (lambda i, t=t: held[t][i])
            finish(item, read, ahead)
        return carry

    first = store(items(0)[0])
    for i in range(pairs):
        first(i)
    if rounds > 1:
        lax.fori_loop(0, rounds, one, 0)
    else:
        one(0, 0)


def main_kernel(dims, pts_hbm, order_hbm, masks_hbm, counts_hbm, gain_hbm, shift_hbm, w_hbm,
                w_out_hbm, tiled_ref, acc_ref, l_ref, live_ref, w_out_ref, done_ref, pts_ref, order_ref,
                attn_ref, normed_ref, block_ref, kv_ref, pick_ref, qd_ref, tag_ref, s_ref, m_ref, gain_ref, shift_ref, w_ref, on_ref,
                masks_ref, counts_ref, sems, own_sem, pair_send, pair_recv, far_send, far_recv):
    by, bz, p, width, n = dims
    nb = by * bz
    hd = width // HEADS
    me = lax.axis_index("gx")
    odd = me % 2
    pair = me + 1 - 2 * odd
    far = me - 1 + 2 * odd
    has = (far >= 0) & (far < n)
    barrier = pltpu.get_barrier_semaphore()
    pl.semaphore_signal(barrier, inc=1, device_id={"gx": pair}, device_id_type=MESH)

    @pl.when(has)
    def _():
        pl.semaphore_signal(barrier, inc=1, device_id={"gx": far}, device_id_type=MESH)

    small = [
        pltpu.make_async_copy(order_hbm, order_ref.at[0], sems.at[0]),
        pltpu.make_async_copy(gain_hbm, gain_ref, sems.at[1]),
        pltpu.make_async_copy(shift_hbm, shift_ref, sems.at[2]),
        pltpu.make_async_copy(masks_hbm, masks_ref, sems.at[3]),
        pltpu.make_async_copy(counts_hbm, counts_ref, sems.at[4]),
    ]
    own = pltpu.make_async_copy(pts_hbm, pts_ref.at[0], own_sem)
    weights = pltpu.make_async_copy(w_hbm, w_ref, sems.at[5])
    weights_out = pltpu.make_async_copy(w_out_hbm, w_out_ref, sems.at[6])
    for copy in small + [own, weights, weights_out]:
        copy.start()

    def send(source, target, out_sem, in_sem, device):
        return pltpu.make_async_remote_copy(
            src_ref=source, dst_ref=target, send_sem=out_sem, recv_sem=in_sem,
            device_id={"gx": device}, device_id_type=MESH,
        )

    def far_block(k):
        return send(pts_hbm.at[k], pts_ref.at[2, k], far_send.at[k], far_recv.at[k], far)

    far_order = send(order_hbm, order_ref.at[2], far_send.at[nb], far_recv.at[nb], far)
    pair_order = send(order_hbm, order_ref.at[1], pair_send.at[0], pair_recv.at[0], pair)
    pair_points = send(pts_hbm, pts_ref.at[1], pair_send.at[1], pair_recv.at[1], pair)

    @pl.when(has)
    def _():
        pl.semaphore_wait(barrier, 2)

    @pl.when(jnp.logical_not(has))
    def _():
        pl.semaphore_wait(barrier, 1)

    @pl.when(has)
    def _():
        far_order.start()
        for k in range(nb):
            far_block(k).start()

    pair_order.start()
    pair_points.start()

    for copy in small:
        copy.wait()
    near = reach(by, bz)
    reachable = len(near)
    here = has.astype(jnp.int32)
    slabs = [(me, 1), (pair, 1), ((far + n) % n, here)]
    row = lax.broadcasted_iota(jnp.int32, (p, 2 * p), 0)
    lane = lax.broadcasted_iota(jnp.int32, (p, p), 1)
    same = jnp.where(lax.broadcasted_iota(jnp.int32, (p, p), 0) == lane, 1.0, 0.0)
    for s, (at, there) in enumerate(slabs):
        for g in range(nb):
            j, l = spot(g, bz)
            tag_ref[s, g] = jnp.where(row < counts_ref[j, l, at], 0.0, NEG).astype(jnp.bfloat16)
            if s == 0:
                pick_ref[0, g] = same.astype(jnp.bfloat16)
            for r, (b, c) in enumerate(near):
                inside = 0 <= j + b < by and 0 <= l + c < bz
                key = g if s < 2 else (g + b * bz + c) % nb
                on = there if inside else 0
                if inside and s == 0 and (b, c) != (0, 0):
                    on = masks_ref[0, j, l, column_of(0, b, c)]
                if inside and s > 0:
                    plus, minus = column_of(1, b, c), column_of(-1, b, c)
                    sign = 1 - odd if s == 1 else odd
                    on = masks_ref[0, j, l, minus + (plus - minus) * sign] * there
                on_ref[(s * nb + key) * reachable + r] = on
    for g in range(nb):
        j, l = spot(g, bz)
        live_ref[g] = jnp.full(live_ref.shape[1:], counts_ref[j, l, me], jnp.int32)
    acc_ref[...] = jnp.zeros_like(acc_ref)
    l_ref[...] = jnp.zeros_like(l_ref)
    m_ref[...] = jnp.full_like(m_ref, NEG)

    own.wait()
    for g in range(nb):
        tiled = lax.dot_general(
            chosen(order_ref.at[0], g, bz, p), pts_ref[0, g], (((0,), (0,)), ((), ())),
            preferred_element_type=jnp.float32,
        )
        tiled_ref[g] = tiled.astype(jnp.bfloat16)
        normed_ref[g * p : (g + 1) * p, :] = norm(tiled, gain_ref, shift_ref)
    weights.wait()
    weights_out.wait()
    blank = jnp.zeros((hd, p), jnp.bfloat16)

    def put_q(col, part):
        part = part.astype(jnp.bfloat16) * jnp.bfloat16(1.0 / hd**0.5)
        for g in range(nb):
            turned = part[g * p : (g + 1) * p, :].T
            for h in range(TILE // hd):
                i, k = (col // hd + h) // 2, h % 2
                down = slice(k * hd, (k + 1) * hd)
                qd_ref[g, i, down, k * p : (k + 1) * p] = turned[h * hd : (h + 1) * hd, :]
                qd_ref[g, i, down, (1 - k) * p : (2 - k) * p] = blank

    project(normed_ref, w_ref, 0, width, put_q)
    project(normed_ref, w_ref, width, 3 * width, put_keys(kv_ref, 0, width))
    rest = (kv_ref, pick_ref, qd_ref, tag_ref, s_ref, on_ref, m_ref, l_ref, acc_ref, width, p)

    def around(s):
        def items(g):
            return [(s, k, g, (s * nb + g) * reachable + r) for r, g, k in links(by, bz, g, 1)]

        def row(u):
            places = [u * per + t + 1 for t in range(per)]
            return [(s, v // 3 + v % 3 - 1, v // 3, s * nb * 3 + v) for v in places]

        if bz > 1 or by == 1:
            return nb, items
        per = max(d for d in (1, 2, 4) if (3 * nb - 2) % d == 0)
        return (3 * nb - 2) // per, row

    flow(*around(0), *rest)
    pair_order.wait_recv()
    pair_points.wait_recv()
    for g in range(nb):
        pick_ref[1, g] = chosen(order_ref.at[1], g, bz, p)
        normed_ref[g * p : (g + 1) * p, :] = norm(pts_ref[1, g], gain_ref, shift_ref)
    project(normed_ref, w_ref, width, 3 * width, put_keys(kv_ref, 1, width))
    flow(*around(1), *rest)

    def fetch(k):
        far_block(k).wait_recv()
        pick_ref[2, k] = chosen(order_ref.at[2], k, bz, p)
        block_ref[...] = norm(pts_ref[2, k], gain_ref, shift_ref)
        for col in range(width, 3 * width, TILE):
            part = jnp.dot(
                block_ref[...], w_ref[:, col : col + TILE], preferred_element_type=jnp.float32
            )
            kv_ref[2, k, :, col - width : col - width + TILE] = part.astype(jnp.bfloat16)

    def served(k):
        def items(u):
            return [(2, k, g, (2 * nb + k) * reachable + r) for r, k, g in links(by, bz, k, -1)]

        flow(1, items, *rest)

    @pl.when(has)
    def _():
        far_order.wait_recv()

        def step(k, carry):
            fetch(k)
            served(k)
            return carry

        lax.fori_loop(0, nb - 1, step, 0)

    early = range(settled(by, bz))
    close(early, early, dims, acc_ref, l_ref, tiled_ref, live_ref, w_out_ref, attn_ref, done_ref)

    @pl.when(has)
    def _():
        fetch(nb - 1)
        served(nb - 1)
        far_order.wait_send()
        for k in range(nb):
            far_block(k).wait_send()

    pair_order.wait_send()
    pair_points.wait_send()


def settled(by, bz):
    return max(by * bz - 1 - max(b * bz + c for b, c in reach(by, bz)), 0)


def close(some, slots, dims, acc_ref, l_ref, tiled_ref, live_ref, w_out_ref, attn_ref, out_ref):
    by, bz, p, width, n = dims
    if not some:
        return
    hd = width // HEADS
    row = lax.broadcasted_iota(jnp.int32, (p, width), 0)
    for t, g in enumerate(some):
        inverse = 1.0 / l_ref[g]
        parts = [
            (acc_ref[g, h * hd : (h + 1) * hd, :] * inverse[h : h + 1, :]).astype(jnp.bfloat16)
            for h in range(HEADS)
        ]
        attn_ref[t * p : (t + 1) * p, :] = jnp.concatenate(parts, axis=0).T
    mixed = jnp.dot(
        attn_ref[: len(some) * p, :], w_out_ref[...], preferred_element_type=jnp.float32
    )
    for t, (g, slot) in enumerate(zip(some, slots)):
        part = mixed[t * p : (t + 1) * p] + tiled_ref[g].astype(jnp.float32)
        part = jnp.where(row < live_ref[g, :1, :], part, 0.0)
        out_ref[slot] = part.astype(jnp.bfloat16)


def tail_kernel(dims, acc_ref, l_ref, tiled_ref, live_ref, w_out_ref, done_ref, out_hbm, attn_ref,
                out_ref, sems):
    by, bz, p, width, n = dims
    nb = by * bz
    early = settled(by, bz)
    ends = []

    def send(source, lo, size):
        end = pltpu.make_async_copy(source, out_hbm.at[pl.ds(lo, size)], sems.at[len(ends)])
        end.start()
        ends.append(end)

    if early:
        send(done_ref, 0, early)
    late = range(early, nb)
    close(late, range(len(late)), dims, acc_ref, l_ref, tiled_ref, live_ref, w_out_ref, attn_ref,
          out_ref)
    send(out_ref, early, len(late))
    for end in ends:
        end.wait()


def shards(points, order, masks, counts, gain, shift_bias, w_qkv, w_out):
    _, by, bz, p, width = points.shape
    n = lax.axis_size("gx")
    nb = by * bz
    dims = (by, bz, p, width, n)
    counts = counts.transpose(1, 2, 0)
    pin = lambda value: pltpu.with_memory_space_constraint(value, pltpu.HBM)
    shape = jax.ShapeDtypeStruct
    dma = pltpu.SemaphoreType.DMA
    vmem = pl.BlockSpec(memory_space=pltpu.VMEM)
    hbm = pl.BlockSpec(memory_space=pltpu.HBM)
    half = jnp.bfloat16
    early = settled(by, bz)
    tiled, acc, sums, live, w_here, done = pl.pallas_call(
        functools.partial(main_kernel, dims),
        name="main",
        out_shape=[
            shape((nb, p, width), half),
            shape((nb, width, p), jnp.float32),
            shape((nb, HEADS, p), jnp.float32),
            shape((nb, 8, width), jnp.int32),
            shape(w_out.shape, half),
            shape((max(early, 1), p, width), half),
        ],
        in_specs=[hbm] * 8,
        out_specs=[vmem] * 6,
        scratch_shapes=[
            pltpu.VMEM((3, nb, p, width), half),
            pltpu.VMEM((3,) + order.shape, jnp.int32),
            pltpu.VMEM((max(early, 1) * p, width), half),
            pltpu.VMEM((nb * p, width), half),
            pltpu.VMEM((p, width), half),
            pltpu.VMEM((3, nb, p, 2 * width), half),
            pltpu.VMEM((3, nb, p, p), half),
            pltpu.VMEM((nb, HEADS // 2, width // HEADS * 2, 2 * p), half),
            pltpu.VMEM((3, nb, p, 2 * p), half),
            pltpu.VMEM((HEADS // 2, p, 2 * p), jnp.float32),
            pltpu.VMEM((nb, HEADS, p), jnp.float32),
            pltpu.VMEM((1, width), jnp.float32),
            pltpu.VMEM((1, width), jnp.float32),
            pltpu.VMEM(w_qkv.shape, half),
            pltpu.SMEM((3 * nb * len(reach(by, bz)),), jnp.int32),
            pltpu.SMEM(masks.shape, jnp.int32),
            pltpu.SMEM(counts.shape, jnp.int32),
            dma((7,)),
            dma,
            dma((2,)),
            dma((2,)),
            dma((nb + 1,)),
            dma((nb + 1,)),
        ],
        cost_estimate=pl.CostEstimate(
            flops=2 * nb * p * width * 24 * width, transcendentals=0, bytes_accessed=8 << 20
        ),
        compiler_params=pltpu.CompilerParams(
            vmem_limit_bytes=48 << 20, collective_id=0, has_side_effects=True
        ),
    )(
        pin(points.reshape(nb, p, width)),
        pin(order),
        pin(masks),
        pin(counts),
        pin(gain.reshape(1, width)),
        pin(shift_bias.reshape(1, width)),
        pin(w_qkv),
        pin(w_out),
    )
    out = pl.pallas_call(
        functools.partial(tail_kernel, dims),
        name="tail",
        out_shape=shape((nb, p, width), half),
        in_specs=[vmem] * 6,
        out_specs=hbm,
        scratch_shapes=[
            pltpu.VMEM(((nb - early) * p, width), half),
            pltpu.VMEM((nb - early, p, width), half),
            dma((2,)),
        ],
        cost_estimate=pl.CostEstimate(
            flops=2 * (nb - early) * p * width * width, transcendentals=0, bytes_accessed=2 << 20
        ),
        compiler_params=pltpu.CompilerParams(vmem_limit_bytes=16 << 20),
    )(acc, sums, tiled, live, w_here, done)
    return out.reshape(points.shape)


def solution(mesh):
    placed = (
        P(("groups", "gx"), None, None, None, None),
        P(("groups", "gx"), None, None, None),
        P(("groups", "gx"), None, None, None),
        P("groups", None, None),
        P(),
        P(),
        P(),
        P(),
    )
    return jax.shard_map(
        shards,
        mesh=mesh,
        in_specs=placed,
        out_specs=P(("groups", "gx"), None, None, None, None),
        check_vma=False,
    )
```

```python
import functools

import jax
import jax.numpy as jnp
from jax import lax
from jax.experimental import pallas as pl
from jax.experimental.pallas import tpu as pltpu
from jax.sharding import PartitionSpec as P

HEADS = 8
TILE = 256
NEG = -1e30
OFF = -3e30
ONES = 16
MESH = pl.DeviceIdType.MESH


def column_of(a, b, c):
    index = 9 * (a + 1) + 3 * (b + 1) + (c + 1)
    return index if index < 13 else index - 1


def reach(by, bz):
    spans = [(b, c) for b in (-1, 0, 1) for c in (-1, 0, 1)]
    return [o for o in spans if (by > 1 or o[0] == 0) and (bz > 1 or o[1] == 0)]


def links(by, bz, k, side):
    nb = by * bz
    found = []
    for r, (b, c) in enumerate(reach(by, bz)):
        if isinstance(k, int):
            j, l = k // bz + side * b, k % bz + side * c
            if not (0 <= j < by and 0 <= l < bz):
                continue
        other = (k + side * (b * bz + c) + nb) % nb
        found.append((r, k, other))
    return found


def spot(k, bz):
    return (k, 0) if bz == 1 else (k // bz, k % bz)


def chosen(order_ref, k, bz, p):
    j, l = spot(k, bz)
    row = order_ref[0, j, pl.ds(l, 1), :]
    pick = lax.broadcasted_iota(jnp.int32, (p, p), 0) == row
    return jnp.where(pick, 1.0, 0.0).astype(jnp.bfloat16)


def norm(values, gain_ref, shift_ref):
    values = values.astype(jnp.float32)
    mean = jnp.mean(values, axis=-1, keepdims=True)
    away = values - mean
    var = jnp.mean(away * away, axis=-1, keepdims=True)
    normed = away * lax.rsqrt(var + 1e-05) * gain_ref[...] + shift_ref[...]
    return normed.astype(jnp.bfloat16)


def project(normed_ref, w_ref, lo, hi, put):
    for col in range(lo, hi, TILE):
        part = jnp.dot(
            normed_ref[...], w_ref[:, col : col + TILE], preferred_element_type=jnp.float32
        )
        put(col, part)


def put_keys(kv_ref, s, width):
    def put(col, part):
        nb, p = kv_ref.shape[1:3]
        part = part.astype(jnp.bfloat16).reshape(nb, p, TILE)
        kv_ref[s, :, :, col - width : col - width + TILE] = part

    return put


def flow(rounds, items, kv_ref, pick_ref, qd_ref, tag_ref, s_ref, on_ref, m_ref, l_ref, acc_ref, width, p):
    hd = width // HEADS
    pairs = HEADS // 2

    def lanes_of(both, i):
        return jnp.concatenate([both[2 * i : 2 * i + 1], both[2 * i + 1 : 2 * i + 2]], axis=1)

    def scores(item, i):
        s, k, g, at = item
        keys = jnp.concatenate(
            [kv_ref[s, k, :, 2 * i * hd : 2 * (i + 1) * hd], pick_ref[s, k]], axis=1
        )
        asked = jnp.concatenate([qd_ref[g, i], tag_ref[s, k]], axis=0)
        return jnp.dot(keys, asked, preferred_element_type=jnp.float32)

    def soften(item, state, i, s):
        off = jnp.where(on_ref[item[3]] == 1, 0.0, OFF)
        old = lanes_of(state, i)
        top = jnp.maximum(old, jnp.max(s, axis=0, keepdims=True) + off)
        keep = jnp.exp(old - top)
        e = jnp.exp(s - (top - off))
        return top, keep, e.astype(jnp.bfloat16)

    def mix(item, i, e):
        values = kv_ref[item[0], item[1], :, width + 2 * i * hd : width + 2 * (i + 1) * hd]
        lines = jnp.concatenate([values.T, jnp.ones((ONES, p), jnp.bfloat16)], axis=0)
        return jnp.dot(lines, e, preferred_element_type=jnp.float32)

    def put(item, i, soft, out):
        g = item[2]
        top, keep, _ = soft
        mass = out[2 * hd : 2 * hd + 1, :]
        for k in range(2):
            h = 2 * i + k
            lanes = slice(k * p, (k + 1) * p)
            down = slice(h * hd, (h + 1) * hd)
            old = acc_ref[g, down, :] * keep[:, lanes]
            acc_ref[g, down, :] = old + out[k * hd : (k + 1) * hd, lanes]
            l_ref[g, h : h + 1, :] = l_ref[g, h : h + 1, :] * keep[:, lanes] + mass[:, lanes]
            m_ref[g, h : h + 1, :] = top[:, lanes]

    def finish(item, read, ahead):
        state = m_ref[item[2]]
        last = None
        for i in range(pairs):
            ahead(i)
            soft = soften(item, state, i, read(i))
            out = mix(item, i, soft[2])
            if last is not None:
                put(item, *last)
            last = (i, soft, out)
        put(item, *last)

    def store(item):
        def ahead(i):
            s_ref[i] = scores(item, i)

        return ahead

    def one(u, carry):
        now = items(u)
        after = items((u + 1) % rounds)[0] if rounds > 1 else None
        held = [{} for _ in now]
        for t, item in enumerate(now):
            if t + 1 < len(now):
                ahead = lambda i, t=t: held[t + 1].update({i: scores(now[t + 1], i)})
            elif after is not None:
                ahead = store(after)
            else:
                ahead = lambda i: None
            read = (lambda i: s_ref[i]) if t == 0 else (lambda i, t=t: held[t][i])
            finish(item, read, ahead)
        return carry

    first = store(items(0)[0])
    for i in range(pairs):
        first(i)
    if rounds > 1:
        lax.fori_loop(0, rounds, one, 0)
    else:
        one(0, 0)


def main_kernel(dims, pts_hbm, order_hbm, masks_hbm, counts_hbm, gain_hbm, shift_hbm, w_hbm,
                w_out_hbm, tiled_ref, acc_ref, l_ref, live_ref, w_out_ref, done_ref, pts_ref, order_ref,
                attn_ref, normed_ref, block_ref, kv_ref, pick_ref, qd_ref, tag_ref, s_ref, m_ref, gain_ref, shift_ref, w_ref, on_ref,
                masks_ref, counts_ref, sems, own_sem, pair_send, pair_recv, far_send, far_recv):
    by, bz, p, width, n = dims
    nb = by * bz
    hd = width // HEADS
    me = lax.axis_index("gx")
    odd = me % 2
    pair = me + 1 - 2 * odd
    far = me - 1 + 2 * odd
    has = (far >= 0) & (far < n)
    barrier = pltpu.get_barrier_semaphore()
    pl.semaphore_signal(barrier, inc=1, device_id={"gx": pair}, device_id_type=MESH)

    @pl.when(has)
    def _():
        pl.semaphore_signal(barrier, inc=1, device_id={"gx": far}, device_id_type=MESH)

    small = [
        pltpu.make_async_copy(order_hbm, order_ref.at[0], sems.at[0]),
        pltpu.make_async_copy(gain_hbm, gain_ref, sems.at[1]),
        pltpu.make_async_copy(shift_hbm, shift_ref, sems.at[2]),
        pltpu.make_async_copy(masks_hbm, masks_ref, sems.at[3]),
        pltpu.make_async_copy(counts_hbm, counts_ref, sems.at[4]),
    ]
    own = pltpu.make_async_copy(pts_hbm, pts_ref.at[0], own_sem)
    weights = pltpu.make_async_copy(w_hbm, w_ref, sems.at[5])
    weights_out = pltpu.make_async_copy(w_out_hbm, w_out_ref, sems.at[6])
    for copy in small + [own, weights, weights_out]:
        copy.start()

    def send(source, target, out_sem, in_sem, device):
        return pltpu.make_async_remote_copy(
            src_ref=source, dst_ref=target, send_sem=out_sem, recv_sem=in_sem,
            device_id={"gx": device}, device_id_type=MESH,
        )

    def far_block(k):
        return send(pts_hbm.at[k], pts_ref.at[2, k], far_send.at[k], far_recv.at[k], far)

    far_order = send(order_hbm, order_ref.at[2], far_send.at[nb], far_recv.at[nb], far)
    pair_order = send(order_hbm, order_ref.at[1], pair_send.at[0], pair_recv.at[0], pair)
    pair_points = send(pts_hbm, pts_ref.at[1], pair_send.at[1], pair_recv.at[1], pair)

    @pl.when(has)
    def _():
        pl.semaphore_wait(barrier, 2)

    @pl.when(jnp.logical_not(has))
    def _():
        pl.semaphore_wait(barrier, 1)

    @pl.when(has)
    def _():
        far_block(0).start()
        far_order.start()
        for k in range(1, nb):
            far_block(k).start()

    pair_order.start()
    pair_points.start()

    for copy in small:
        copy.wait()
    near = reach(by, bz)
    reachable = len(near)
    here = has.astype(jnp.int32)
    slabs = [(me, 1), (pair, 1), ((far + n) % n, here)]
    row = lax.broadcasted_iota(jnp.int32, (p, 2 * p), 0)
    lane = lax.broadcasted_iota(jnp.int32, (p, p), 1)
    same = jnp.where(lax.broadcasted_iota(jnp.int32, (p, p), 0) == lane, 1.0, 0.0)
    for s, (at, there) in enumerate(slabs):
        for g in range(nb):
            j, l = spot(g, bz)
            tag_ref[s, g] = jnp.where(row < counts_ref[j, l, at], 0.0, NEG).astype(jnp.bfloat16)
            if s == 0:
                pick_ref[0, g] = same.astype(jnp.bfloat16)
            for r, (b, c) in enumerate(near):
                inside = 0 <= j + b < by and 0 <= l + c < bz
                key = g if s < 2 else (g + b * bz + c) % nb
                on = there if inside else 0
                if inside and s == 0 and (b, c) != (0, 0):
                    on = masks_ref[0, j, l, column_of(0, b, c)]
                if inside and s > 0:
                    plus, minus = column_of(1, b, c), column_of(-1, b, c)
                    sign = 1 - odd if s == 1 else odd
                    on = masks_ref[0, j, l, minus + (plus - minus) * sign] * there
                on_ref[(s * nb + key) * reachable + r] = on
    for g in range(nb):
        j, l = spot(g, bz)
        live_ref[g] = jnp.full(live_ref.shape[1:], counts_ref[j, l, me], jnp.int32)
    acc_ref[...] = jnp.zeros_like(acc_ref)
    l_ref[...] = jnp.zeros_like(l_ref)
    m_ref[...] = jnp.full_like(m_ref, NEG)

    own.wait()
    for g in range(nb):
        tiled = lax.dot_general(
            chosen(order_ref.at[0], g, bz, p), pts_ref[0, g], (((0,), (0,)), ((), ())),
            preferred_element_type=jnp.float32,
        )
        tiled_ref[g] = tiled.astype(jnp.bfloat16)
        normed_ref[g * p : (g + 1) * p, :] = norm(tiled, gain_ref, shift_ref)
    weights.wait()
    weights_out.wait()
    blank = jnp.zeros((hd, p), jnp.bfloat16)

    def put_q(col, part):
        part = part.astype(jnp.bfloat16) * jnp.bfloat16(1.0 / hd**0.5)
        for g in range(nb):
            turned = part[g * p : (g + 1) * p, :].T
            for h in range(TILE // hd):
                i, k = (col // hd + h) // 2, h % 2
                down = slice(k * hd, (k + 1) * hd)
                qd_ref[g, i, down, k * p : (k + 1) * p] = turned[h * hd : (h + 1) * hd, :]
                qd_ref[g, i, down, (1 - k) * p : (2 - k) * p] = blank

    project(normed_ref, w_ref, 0, width, put_q)
    project(normed_ref, w_ref, width, 3 * width, put_keys(kv_ref, 0, width))
    rest = (kv_ref, pick_ref, qd_ref, tag_ref, s_ref, on_ref, m_ref, l_ref, acc_ref, width, p)

    def around(s):
        def items(g):
            return [(s, k, g, (s * nb + g) * reachable + r) for r, g, k in links(by, bz, g, 1)]

        def row(u):
            places = [u * per + t + 1 for t in range(per)]
            return [(s, v // 3 + v % 3 - 1, v // 3, s * nb * 3 + v) for v in places]

        if bz > 1 or by == 1:
            return nb, items
        per = max(d for d in (1, 2, 4) if (3 * nb - 2) % d == 0)
        return (3 * nb - 2) // per, row

    flow(*around(0), *rest)
    pair_order.wait_recv()
    pair_points.wait_recv()
    for g in range(nb):
        pick_ref[1, g] = chosen(order_ref.at[1], g, bz, p)
        normed_ref[g * p : (g + 1) * p, :] = norm(pts_ref[1, g], gain_ref, shift_ref)
    project(normed_ref, w_ref, width, 3 * width, put_keys(kv_ref, 1, width))
    flow(*around(1), *rest)

    def fetch(k):
        far_block(k).wait_recv()
        pick_ref[2, k] = chosen(order_ref.at[2], k, bz, p)
        block_ref[...] = norm(pts_ref[2, k], gain_ref, shift_ref)
        for col in range(width, 3 * width, TILE):
            part = jnp.dot(
                block_ref[...], w_ref[:, col : col + TILE], preferred_element_type=jnp.float32
            )
            kv_ref[2, k, :, col - width : col - width + TILE] = part.astype(jnp.bfloat16)

    def served(k):
        def items(u):
            return [(2, k, g, (2 * nb + k) * reachable + r) for r, k, g in links(by, bz, k, -1)]

        flow(1, items, *rest)

    @pl.when(has)
    def _():
        far_order.wait_recv()

        def step(k, carry):
            fetch(k)
            served(k)
            return carry

        lax.fori_loop(0, nb - 1, step, 0)

    early = range(settled(by, bz))
    close(early, early, dims, acc_ref, l_ref, tiled_ref, live_ref, w_out_ref, attn_ref, done_ref)

    @pl.when(has)
    def _():
        fetch(nb - 1)
        served(nb - 1)
        far_order.wait_send()
        for k in range(nb):
            far_block(k).wait_send()

    pair_order.wait_send()
    pair_points.wait_send()


def settled(by, bz):
    return max(by * bz - 1 - max(b * bz + c for b, c in reach(by, bz)), 0)


def close(some, slots, dims, acc_ref, l_ref, tiled_ref, live_ref, w_out_ref, attn_ref, out_ref):
    by, bz, p, width, n = dims
    if not some:
        return
    hd = width // HEADS
    row = lax.broadcasted_iota(jnp.int32, (p, width), 0)
    for t, g in enumerate(some):
        inverse = 1.0 / l_ref[g]
        parts = [
            (acc_ref[g, h * hd : (h + 1) * hd, :] * inverse[h : h + 1, :]).astype(jnp.bfloat16)
            for h in range(HEADS)
        ]
        attn_ref[t * p : (t + 1) * p, :] = jnp.concatenate(parts, axis=0).T
    mixed = jnp.dot(
        attn_ref[: len(some) * p, :], w_out_ref[...], preferred_element_type=jnp.float32
    )
    for t, (g, slot) in enumerate(zip(some, slots)):
        part = mixed[t * p : (t + 1) * p] + tiled_ref[g].astype(jnp.float32)
        part = jnp.where(row < live_ref[g, :1, :], part, 0.0)
        out_ref[slot] = part.astype(jnp.bfloat16)


def tail_kernel(dims, acc_ref, l_ref, tiled_ref, live_ref, w_out_ref, done_ref, out_hbm, attn_ref,
                out_ref, sems):
    by, bz, p, width, n = dims
    nb = by * bz
    early = settled(by, bz)
    ends = []

    def send(source, lo, size):
        end = pltpu.make_async_copy(source, out_hbm.at[pl.ds(lo, size)], sems.at[len(ends)])
        end.start()
        ends.append(end)

    if early:
        send(done_ref, 0, early)
    for t, g in enumerate(range(early, nb)):
        close([g], [t], dims, acc_ref, l_ref, tiled_ref, live_ref, w_out_ref,
              attn_ref.at[pl.ds(t * p, p)], out_ref)
        send(out_ref.at[pl.ds(t, 1)], g, 1)
    for end in ends:
        end.wait()


def shards(points, order, masks, counts, gain, shift_bias, w_qkv, w_out):
    _, by, bz, p, width = points.shape
    n = lax.axis_size("gx")
    nb = by * bz
    dims = (by, bz, p, width, n)
    counts = counts.transpose(1, 2, 0)
    pin = lambda value: pltpu.with_memory_space_constraint(value, pltpu.HBM)
    shape = jax.ShapeDtypeStruct
    dma = pltpu.SemaphoreType.DMA
    vmem = pl.BlockSpec(memory_space=pltpu.VMEM)
    hbm = pl.BlockSpec(memory_space=pltpu.HBM)
    half = jnp.bfloat16
    early = settled(by, bz)
    tiled, acc, sums, live, w_here, done = pl.pallas_call(
        functools.partial(main_kernel, dims),
        name="main",
        out_shape=[
            shape((nb, p, width), half),
            shape((nb, width, p), jnp.float32),
            shape((nb, HEADS, p), jnp.float32),
            shape((nb, 8, width), jnp.int32),
            shape(w_out.shape, half),
            shape((max(early, 1), p, width), half),
        ],
        in_specs=[hbm] * 8,
        out_specs=[vmem] * 6,
        scratch_shapes=[
            pltpu.VMEM((3, nb, p, width), half),
            pltpu.VMEM((3,) + order.shape, jnp.int32),
            pltpu.VMEM((max(early, 1) * p, width), half),
            pltpu.VMEM((nb * p, width), half),
            pltpu.VMEM((p, width), half),
            pltpu.VMEM((3, nb, p, 2 * width), half),
            pltpu.VMEM((3, nb, p, p), half),
            pltpu.VMEM((nb, HEADS // 2, width // HEADS * 2, 2 * p), half),
            pltpu.VMEM((3, nb, p, 2 * p), half),
            pltpu.VMEM((HEADS // 2, p, 2 * p), jnp.float32),
            pltpu.VMEM((nb, HEADS, p), jnp.float32),
            pltpu.VMEM((1, width), jnp.float32),
            pltpu.VMEM((1, width), jnp.float32),
            pltpu.VMEM(w_qkv.shape, half),
            pltpu.SMEM((3 * nb * len(reach(by, bz)),), jnp.int32),
            pltpu.SMEM(masks.shape, jnp.int32),
            pltpu.SMEM(counts.shape, jnp.int32),
            dma((7,)),
            dma,
            dma((2,)),
            dma((2,)),
            dma((nb + 1,)),
            dma((nb + 1,)),
        ],
        cost_estimate=pl.CostEstimate(
            flops=2 * nb * p * width * 24 * width, transcendentals=0, bytes_accessed=8 << 20
        ),
        compiler_params=pltpu.CompilerParams(
            vmem_limit_bytes=48 << 20, collective_id=0, has_side_effects=True
        ),
    )(
        pin(points.reshape(nb, p, width)),
        pin(order),
        pin(masks),
        pin(counts),
        pin(gain.reshape(1, width)),
        pin(shift_bias.reshape(1, width)),
        pin(w_qkv),
        pin(w_out),
    )
    out = pl.pallas_call(
        functools.partial(tail_kernel, dims),
        name="tail",
        out_shape=shape((nb, p, width), half),
        in_specs=[vmem] * 6,
        out_specs=hbm,
        scratch_shapes=[
            pltpu.VMEM(((nb - early) * p, width), half),
            pltpu.VMEM((nb - early, p, width), half),
            dma((1 + nb - early,)),
        ],
        cost_estimate=pl.CostEstimate(
            flops=2 * (nb - early) * p * width * width, transcendentals=0, bytes_accessed=2 << 20
        ),
        compiler_params=pltpu.CompilerParams(vmem_limit_bytes=16 << 20),
    )(acc, sums, tiled, live, w_here, done)
    return out.reshape(points.shape)


def solution(mesh):
    placed = (
        P(("groups", "gx"), None, None, None, None),
        P(("groups", "gx"), None, None, None),
        P(("groups", "gx"), None, None, None),
        P("groups", None, None),
        P(),
        P(),
        P(),
        P(),
    )
    return jax.shard_map(
        shards,
        mesh=mesh,
        in_specs=placed,
        out_specs=P(("groups", "gx"), None, None, None, None),
        check_vma=False,
    )
```

```python
import functools

import jax
import jax.numpy as jnp
from jax import lax
from jax.experimental import pallas as pl
from jax.experimental.pallas import tpu as pltpu
from jax.sharding import PartitionSpec as P

HEADS = 8
TILE = 256
NEG = -1e30
OFF = -3e30
ONES = 16
MESH = pl.DeviceIdType.MESH


def column_of(a, b, c):
    index = 9 * (a + 1) + 3 * (b + 1) + (c + 1)
    return index if index < 13 else index - 1


def reach(by, bz):
    spans = [(b, c) for b in (-1, 0, 1) for c in (-1, 0, 1)]
    return [o for o in spans if (by > 1 or o[0] == 0) and (bz > 1 or o[1] == 0)]


def links(by, bz, k, side):
    nb = by * bz
    found = []
    for r, (b, c) in enumerate(reach(by, bz)):
        if isinstance(k, int):
            j, l = k // bz + side * b, k % bz + side * c
            if not (0 <= j < by and 0 <= l < bz):
                continue
        other = (k + side * (b * bz + c) + nb) % nb
        found.append((r, k, other))
    return found


def spot(k, bz):
    return (k, 0) if bz == 1 else (k // bz, k % bz)


def chosen(order_ref, k, bz, p):
    j, l = spot(k, bz)
    row = order_ref[0, j, pl.ds(l, 1), :]
    pick = lax.broadcasted_iota(jnp.int32, (p, p), 0) == row
    return jnp.where(pick, 1.0, 0.0).astype(jnp.bfloat16)


def norm(values, gain_ref, shift_ref):
    values = values.astype(jnp.float32)
    mean = jnp.mean(values, axis=-1, keepdims=True)
    away = values - mean
    var = jnp.mean(away * away, axis=-1, keepdims=True)
    normed = away * lax.rsqrt(var + 1e-05) * gain_ref[...] + shift_ref[...]
    return normed.astype(jnp.bfloat16)


def project(normed_ref, w_ref, lo, hi, put):
    for col in range(lo, hi, TILE):
        part = jnp.dot(
            normed_ref[...], w_ref[:, col : col + TILE], preferred_element_type=jnp.float32
        )
        put(col, part)


def put_keys(kv_ref, s, width):
    def put(col, part):
        nb, p = kv_ref.shape[1:3]
        part = part.astype(jnp.bfloat16).reshape(nb, p, TILE)
        kv_ref[s, :, :, col - width : col - width + TILE] = part

    return put


def flow(rounds, items, kv_ref, pick_ref, qd_ref, tag_ref, s_ref, on_ref, m_ref, l_ref, acc_ref, width, p):
    hd = width // HEADS
    pairs = HEADS // 2

    def lanes_of(both, i):
        return jnp.concatenate([both[2 * i : 2 * i + 1], both[2 * i + 1 : 2 * i + 2]], axis=1)

    def scores(item, i):
        s, k, g, at = item
        keys = jnp.concatenate(
            [kv_ref[s, k, :, 2 * i * hd : 2 * (i + 1) * hd], pick_ref[s, k]], axis=1
        )
        asked = jnp.concatenate([qd_ref[g, i], tag_ref[s, k]], axis=0)
        return jnp.dot(keys, asked, preferred_element_type=jnp.float32)

    def soften(item, state, i, s):
        off = jnp.where(on_ref[item[3]] == 1, 0.0, OFF)
        old = lanes_of(state, i)
        top = jnp.maximum(old, jnp.max(s, axis=0, keepdims=True) + off)
        keep = jnp.exp(old - top)
        e = jnp.exp(s - (top - off))
        return top, keep, e.astype(jnp.bfloat16)

    def mix(item, i, e):
        values = kv_ref[item[0], item[1], :, width + 2 * i * hd : width + 2 * (i + 1) * hd]
        lines = jnp.concatenate([values.T, jnp.ones((ONES, p), jnp.bfloat16)], axis=0)
        return jnp.dot(lines, e, preferred_element_type=jnp.float32)

    def put(item, i, soft, out):
        g = item[2]
        top, keep, _ = soft
        mass = out[2 * hd : 2 * hd + 1, :]
        for k in range(2):
            h = 2 * i + k
            lanes = slice(k * p, (k + 1) * p)
            down = slice(h * hd, (h + 1) * hd)
            old = acc_ref[g, down, :] * keep[:, lanes]
            acc_ref[g, down, :] = old + out[k * hd : (k + 1) * hd, lanes]
            l_ref[g, h : h + 1, :] = l_ref[g, h : h + 1, :] * keep[:, lanes] + mass[:, lanes]
            m_ref[g, h : h + 1, :] = top[:, lanes]

    def finish(item, read, ahead):
        state = m_ref[item[2]]
        last = None
        for i in range(pairs):
            ahead(i)
            soft = soften(item, state, i, read(i))
            out = mix(item, i, soft[2])
            if last is not None:
                put(item, *last)
            last = (i, soft, out)
        put(item, *last)

    def store(item):
        def ahead(i):
            s_ref[i] = scores(item, i)

        return ahead

    def one(u, carry):
        now = items(u)
        after = items((u + 1) % rounds)[0] if rounds > 1 else None
        held = [{} for _ in now]
        for t, item in enumerate(now):
            if t + 1 < len(now):
                ahead = lambda i, t=t: held[t + 1].update({i: scores(now[t + 1], i)})
            elif after is not None:
                ahead = store(after)
            else:
                ahead = lambda i: None
            read = (lambda i: s_ref[i]) if t == 0 else (lambda i, t=t: held[t][i])
            finish(item, read, ahead)
        return carry

    first = store(items(0)[0])
    for i in range(pairs):
        first(i)
    if rounds > 1:
        lax.fori_loop(0, rounds, one, 0)
    else:
        one(0, 0)


def main_kernel(dims, pts_hbm, order_hbm, masks_hbm, counts_hbm, gain_hbm, shift_hbm, w_hbm,
                w_out_hbm, tiled_ref, acc_ref, l_ref, live_ref, w_out_ref, done_ref, pts_ref, order_ref,
                attn_ref, normed_ref, block_ref, kv_ref, pick_ref, qd_ref, tag_ref, s_ref, m_ref, gain_ref, shift_ref, w_ref, on_ref,
                masks_ref, counts_ref, sems, own_sem, pair_send, pair_recv, far_send, far_recv):
    by, bz, p, width, n = dims
    nb = by * bz
    hd = width // HEADS
    me = lax.axis_index("gx")
    odd = me % 2
    pair = me + 1 - 2 * odd
    far = me - 1 + 2 * odd
    has = (far >= 0) & (far < n)
    barrier = pltpu.get_barrier_semaphore()
    pl.semaphore_signal(barrier, inc=1, device_id={"gx": pair}, device_id_type=MESH)

    @pl.when(has)
    def _():
        pl.semaphore_signal(barrier, inc=1, device_id={"gx": far}, device_id_type=MESH)

    small = [
        pltpu.make_async_copy(order_hbm, order_ref.at[0], sems.at[0]),
        pltpu.make_async_copy(gain_hbm, gain_ref, sems.at[1]),
        pltpu.make_async_copy(shift_hbm, shift_ref, sems.at[2]),
        pltpu.make_async_copy(masks_hbm, masks_ref, sems.at[3]),
        pltpu.make_async_copy(counts_hbm, counts_ref, sems.at[4]),
    ]
    own = pltpu.make_async_copy(pts_hbm, pts_ref.at[0], own_sem)
    weights = pltpu.make_async_copy(w_hbm, w_ref, sems.at[5])
    weights_out = pltpu.make_async_copy(w_out_hbm, w_out_ref, sems.at[6])
    for copy in small + [own, weights, weights_out]:
        copy.start()

    def send(source, target, out_sem, in_sem, device):
        return pltpu.make_async_remote_copy(
            src_ref=source, dst_ref=target, send_sem=out_sem, recv_sem=in_sem,
            device_id={"gx": device}, device_id_type=MESH,
        )

    def far_block(k):
        return send(pts_hbm.at[k], pts_ref.at[2, k], far_send.at[k], far_recv.at[k], far)

    far_order = send(order_hbm, order_ref.at[2], far_send.at[nb], far_recv.at[nb], far)
    pair_order = send(order_hbm, order_ref.at[1], pair_send.at[0], pair_recv.at[0], pair)
    pair_points = send(pts_hbm, pts_ref.at[1], pair_send.at[1], pair_recv.at[1], pair)

    @pl.when(has)
    def _():
        pl.semaphore_wait(barrier, 2)

    @pl.when(jnp.logical_not(has))
    def _():
        pl.semaphore_wait(barrier, 1)

    @pl.when(has)
    def _():
        far_block(0).start()
        far_order.start()
        for k in range(1, nb):
            far_block(k).start()

    pair_order.start()
    pair_points.start()

    for copy in small:
        copy.wait()
    near = reach(by, bz)
    reachable = len(near)
    here = has.astype(jnp.int32)
    slabs = [(me, 1), (pair, 1), ((far + n) % n, here)]
    row = lax.broadcasted_iota(jnp.int32, (p, 2 * p), 0)
    lane = lax.broadcasted_iota(jnp.int32, (p, p), 1)
    same = jnp.where(lax.broadcasted_iota(jnp.int32, (p, p), 0) == lane, 1.0, 0.0)
    for s, (at, there) in enumerate(slabs):
        for g in range(nb):
            j, l = spot(g, bz)
            tag_ref[s, g] = jnp.where(row < counts_ref[j, l, at], 0.0, NEG).astype(jnp.bfloat16)
            if s == 0:
                pick_ref[0, g] = same.astype(jnp.bfloat16)
            for r, (b, c) in enumerate(near):
                inside = 0 <= j + b < by and 0 <= l + c < bz
                key = g if s < 2 else (g + b * bz + c) % nb
                on = there if inside else 0
                if inside and s == 0 and (b, c) != (0, 0):
                    on = masks_ref[0, j, l, column_of(0, b, c)]
                if inside and s > 0:
                    plus, minus = column_of(1, b, c), column_of(-1, b, c)
                    sign = 1 - odd if s == 1 else odd
                    on = masks_ref[0, j, l, minus + (plus - minus) * sign] * there
                on_ref[(s * nb + key) * reachable + r] = on
    for g in range(nb):
        j, l = spot(g, bz)
        live_ref[g] = jnp.full(live_ref.shape[1:], counts_ref[j, l, me], jnp.int32)
    acc_ref[...] = jnp.zeros_like(acc_ref)
    l_ref[...] = jnp.zeros_like(l_ref)
    m_ref[...] = jnp.full_like(m_ref, NEG)

    own.wait()
    for g in range(nb):
        tiled = lax.dot_general(
            chosen(order_ref.at[0], g, bz, p), pts_ref[0, g], (((0,), (0,)), ((), ())),
            preferred_element_type=jnp.float32,
        )
        tiled_ref[g] = tiled.astype(jnp.bfloat16)
        normed_ref[g * p : (g + 1) * p, :] = norm(tiled, gain_ref, shift_ref)
    weights.wait()
    weights_out.wait()
    blank = jnp.zeros((hd, p), jnp.bfloat16)

    def put_q(col, part):
        part = part.astype(jnp.bfloat16) * jnp.bfloat16(1.0 / hd**0.5)
        for g in range(nb):
            turned = part[g * p : (g + 1) * p, :].T
            for h in range(TILE // hd):
                i, k = (col // hd + h) // 2, h % 2
                down = slice(k * hd, (k + 1) * hd)
                qd_ref[g, i, down, k * p : (k + 1) * p] = turned[h * hd : (h + 1) * hd, :]
                qd_ref[g, i, down, (1 - k) * p : (2 - k) * p] = blank

    project(normed_ref, w_ref, 0, width, put_q)
    project(normed_ref, w_ref, width, 3 * width, put_keys(kv_ref, 0, width))
    rest = (kv_ref, pick_ref, qd_ref, tag_ref, s_ref, on_ref, m_ref, l_ref, acc_ref, width, p)

    def around(s):
        def items(g):
            return [(s, k, g, (s * nb + g) * reachable + r) for r, g, k in links(by, bz, g, 1)]

        def row(u):
            places = [u * per + t + 1 for t in range(per)]
            return [(s, v // 3 + v % 3 - 1, v // 3, s * nb * 3 + v) for v in places]

        if bz > 1 or by == 1:
            return nb, items
        per = max(d for d in (1, 2, 4) if (3 * nb - 2) % d == 0)
        return (3 * nb - 2) // per, row

    flow(*around(0), *rest)
    pair_order.wait_recv()
    pair_points.wait_recv()
    for g in range(nb):
        pick_ref[1, g] = chosen(order_ref.at[1], g, bz, p)
        normed_ref[g * p : (g + 1) * p, :] = norm(pts_ref[1, g], gain_ref, shift_ref)
    project(normed_ref, w_ref, width, 3 * width, put_keys(kv_ref, 1, width))
    flow(*around(1), *rest)

    def fetch(k):
        far_block(k).wait_recv()
        pick_ref[2, k] = chosen(order_ref.at[2], k, bz, p)
        block_ref[...] = norm(pts_ref[2, k], gain_ref, shift_ref)
        for col in range(width, 3 * width, TILE):
            part = jnp.dot(
                block_ref[...], w_ref[:, col : col + TILE], preferred_element_type=jnp.float32
            )
            kv_ref[2, k, :, col - width : col - width + TILE] = part.astype(jnp.bfloat16)

    def served(k):
        def items(u):
            return [(2, k, g, (2 * nb + k) * reachable + r) for r, k, g in links(by, bz, k, -1)]

        flow(1, items, *rest)

    @pl.when(has)
    def _():
        far_order.wait_recv()

        def step(k, carry):
            fetch(k)
            served(k)
            return carry

        lax.fori_loop(0, nb - 2, step, 0)

    early = range(settled(by, bz))
    close(early, early, dims, acc_ref, l_ref, tiled_ref, live_ref, w_out_ref, attn_ref, done_ref)

    @pl.when(has)
    def _():
        for k in range(max(nb - 2, 0), nb):
            fetch(k)
            served(k)
        far_order.wait_send()
        for k in range(nb):
            far_block(k).wait_send()

    pair_order.wait_send()
    pair_points.wait_send()


def settled(by, bz):
    return max(by * bz - 2 - max(b * bz + c for b, c in reach(by, bz)), 0)


def close(some, slots, dims, acc_ref, l_ref, tiled_ref, live_ref, w_out_ref, attn_ref, out_ref):
    by, bz, p, width, n = dims
    if not some:
        return
    hd = width // HEADS
    row = lax.broadcasted_iota(jnp.int32, (p, width), 0)
    for t, g in enumerate(some):
        inverse = 1.0 / l_ref[g]
        parts = [
            (acc_ref[g, h * hd : (h + 1) * hd, :] * inverse[h : h + 1, :]).astype(jnp.bfloat16)
            for h in range(HEADS)
        ]
        attn_ref[t * p : (t + 1) * p, :] = jnp.concatenate(parts, axis=0).T
    mixed = jnp.dot(
        attn_ref[: len(some) * p, :], w_out_ref[...], preferred_element_type=jnp.float32
    )
    for t, (g, slot) in enumerate(zip(some, slots)):
        part = mixed[t * p : (t + 1) * p] + tiled_ref[g].astype(jnp.float32)
        part = jnp.where(row < live_ref[g, :1, :], part, 0.0)
        out_ref[slot] = part.astype(jnp.bfloat16)


def tail_kernel(dims, acc_ref, l_ref, tiled_ref, live_ref, w_out_ref, done_ref, out_hbm, attn_ref,
                out_ref, sems):
    by, bz, p, width, n = dims
    nb = by * bz
    early = settled(by, bz)
    ends = []

    def send(source, lo, size):
        end = pltpu.make_async_copy(source, out_hbm.at[pl.ds(lo, size)], sems.at[len(ends)])
        end.start()
        ends.append(end)

    if early:
        send(done_ref, 0, early)
    for t, g in enumerate(range(early, nb)):
        close([g], [t], dims, acc_ref, l_ref, tiled_ref, live_ref, w_out_ref,
              attn_ref.at[pl.ds(t * p, p)], out_ref)
        send(out_ref.at[pl.ds(t, 1)], g, 1)
    for end in ends:
        end.wait()


def shards(points, order, masks, counts, gain, shift_bias, w_qkv, w_out):
    _, by, bz, p, width = points.shape
    n = lax.axis_size("gx")
    nb = by * bz
    dims = (by, bz, p, width, n)
    counts = counts.transpose(1, 2, 0)
    pin = lambda value: pltpu.with_memory_space_constraint(value, pltpu.HBM)
    shape = jax.ShapeDtypeStruct
    dma = pltpu.SemaphoreType.DMA
    vmem = pl.BlockSpec(memory_space=pltpu.VMEM)
    hbm = pl.BlockSpec(memory_space=pltpu.HBM)
    half = jnp.bfloat16
    early = settled(by, bz)
    tiled, acc, sums, live, w_here, done = pl.pallas_call(
        functools.partial(main_kernel, dims),
        name="main",
        out_shape=[
            shape((nb, p, width), half),
            shape((nb, width, p), jnp.float32),
            shape((nb, HEADS, p), jnp.float32),
            shape((nb, 8, width), jnp.int32),
            shape(w_out.shape, half),
            shape((max(early, 1), p, width), half),
        ],
        in_specs=[hbm] * 8,
        out_specs=[vmem] * 6,
        scratch_shapes=[
            pltpu.VMEM((3, nb, p, width), half),
            pltpu.VMEM((3,) + order.shape, jnp.int32),
            pltpu.VMEM((max(early, 1) * p, width), half),
            pltpu.VMEM((nb * p, width), half),
            pltpu.VMEM((p, width), half),
            pltpu.VMEM((3, nb, p, 2 * width), half),
            pltpu.VMEM((3, nb, p, p), half),
            pltpu.VMEM((nb, HEADS // 2, width // HEADS * 2, 2 * p), half),
            pltpu.VMEM((3, nb, p, 2 * p), half),
            pltpu.VMEM((HEADS // 2, p, 2 * p), jnp.float32),
            pltpu.VMEM((nb, HEADS, p), jnp.float32),
            pltpu.VMEM((1, width), jnp.float32),
            pltpu.VMEM((1, width), jnp.float32),
            pltpu.VMEM(w_qkv.shape, half),
            pltpu.SMEM((3 * nb * len(reach(by, bz)),), jnp.int32),
            pltpu.SMEM(masks.shape, jnp.int32),
            pltpu.SMEM(counts.shape, jnp.int32),
            dma((7,)),
            dma,
            dma((2,)),
            dma((2,)),
            dma((nb + 1,)),
            dma((nb + 1,)),
        ],
        cost_estimate=pl.CostEstimate(
            flops=2 * nb * p * width * 24 * width, transcendentals=0, bytes_accessed=8 << 20
        ),
        compiler_params=pltpu.CompilerParams(
            vmem_limit_bytes=48 << 20, collective_id=0, has_side_effects=True
        ),
    )(
        pin(points.reshape(nb, p, width)),
        pin(order),
        pin(masks),
        pin(counts),
        pin(gain.reshape(1, width)),
        pin(shift_bias.reshape(1, width)),
        pin(w_qkv),
        pin(w_out),
    )
    out = pl.pallas_call(
        functools.partial(tail_kernel, dims),
        name="tail",
        out_shape=shape((nb, p, width), half),
        in_specs=[vmem] * 6,
        out_specs=hbm,
        scratch_shapes=[
            pltpu.VMEM(((nb - early) * p, width), half),
            pltpu.VMEM((nb - early, p, width), half),
            dma((1 + nb - early,)),
        ],
        cost_estimate=pl.CostEstimate(
            flops=2 * (nb - early) * p * width * width, transcendentals=0, bytes_accessed=2 << 20
        ),
        compiler_params=pltpu.CompilerParams(vmem_limit_bytes=16 << 20),
    )(acc, sums, tiled, live, w_here, done)
    return out.reshape(points.shape)


def solution(mesh):
    placed = (
        P(("groups", "gx"), None, None, None, None),
        P(("groups", "gx"), None, None, None),
        P(("groups", "gx"), None, None, None),
        P("groups", None, None),
        P(),
        P(),
        P(),
        P(),
    )
    return jax.shard_map(
        shards,
        mesh=mesh,
        in_specs=placed,
        out_specs=P(("groups", "gx"), None, None, None, None),
        check_vma=False,
    )
```
